16 devices in a mesh: dp: 2 (over y, z), gp: 8 (over x, core).
Axes of the slice: x: 4, y: 2, z: 1, core: 2. Of those that a mesh axis runs over, the one named last changes fastest.
The devices are a block of a 4x4x8 slice.
Arguments:
- x_prev: float32 [65536, 78], P(('dp', 'gp')), parts along dimension 0
- x_cur: float32 [65536, 78], P(('dp', 'gp')), parts along dimension 0
- forcing: float32 [65536, 2, 3], P(('dp', 'gp')), parts along dimension 0
- grid_static: float32 [65536, 3], P(('dp', 'gp')), parts along dimension 0
- g2m_feat: float32 [65536, 4], P(('dp', 'gp')), parts along dimension 0
- m2g_feat: float32 [65536, 4], P(('dp', 'gp')), parts along dimension 0
- mesh_feat: float32 [16384, 3], P(('dp', 'gp')), parts along dimension 0
- mesh_edge_feat: float32 [16384, 6, 4], P(('dp', 'gp')), parts along dimension 0
- norm_stats: float32 [4, 78], replicated
- w_grid_in: bfloat16 [162, 256], replicated
- w_mesh_in: bfloat16 [3, 256], replicated
- w_eemb_in: bfloat16 [3, 4, 256], replicated
- w_embed_out: bfloat16 [5, 256, 256], replicated
- w_edge_in: bfloat16 [18, 768, 256], replicated
- w_edge_out: bfloat16 [18, 256, 256], replicated
- w_node_in: bfloat16 [18, 512, 256], replicated
- w_node_out: bfloat16 [18, 256, 256], replicated
- w_grid_self: bfloat16 [2, 256, 256], replicated
- w_out_hidden: bfloat16 [256, 256], replicated
- w_out_final: bfloat16 [256, 78], replicated
Outputs:
- output 1: float32 [65536, 78], P(('dp', 'gp')), parts along dimension 0
- output 2: float32 [65536, 78], P(('dp', 'gp')), parts along dimension 0
There are 2 independent parts. The reference program is written for one: setup_inputs(seed, part) draws one part's arguments, and reference() takes and returns one part's arrays. A program takes and returns all parts, laid end to end along the dimension named above; an argument that names none is the same for every part.
All inputs are finite; a program needn't handle non-finite values.
Results may differ from the reference program's by a relative error of at most 0.00876042.
Values are sent between devices in bfloat16 or wider.
A program may use at most 768 MiB of HBM per device.

```python
import jax
import jax.numpy as jnp
from jax import lax

GRID_NODES = 32768
MESH_NODES = 8192
SHIFT = 512
LATENT = 256
VARS = 78
FORCE = 3
STATIC = 3
LAYERS = 16
EDGE_FEAT = 4
MESH_FEAT = 3
OFFSET_COUNT = 6

GRID_RATIO = GRID_NODES // MESH_NODES
QUARTER = MESH_NODES // 4
BLOCKS = LAYERS + 2
IN_FEAT = 2 * VARS + FORCE + STATIC
OFFSETS = (1, -1, SHIFT, -SHIFT, QUARTER, -QUARTER)


def normal_weight(key_in, out_shape, fan_in):
    return (jax.random.normal(key_in, out_shape, jnp.float32) * fan_in ** -0.5).astype(jnp.bfloat16)


def setup_inputs(seed: int = 0, part: int = 0) -> dict:
    root_key = jax.random.key(seed)
    part_keys = jax.random.split(jax.random.fold_in(root_key, part), 8)
    weight_keys = jax.random.split(jax.random.key(seed + 1), 15)
    norm_stats = jnp.stack([
        0.5 * jax.random.normal(weight_keys[0], (VARS,), jnp.float32),
        jax.random.uniform(weight_keys[1], (VARS,), jnp.float32, 0.5, 1.5),
        0.2 * jax.random.normal(weight_keys[2], (VARS,), jnp.float32),
        jax.random.uniform(weight_keys[3], (VARS,), jnp.float32, 0.2, 0.6)])
    return {
        "x_prev": jax.random.normal(part_keys[0], (GRID_NODES, VARS), jnp.float32),
        "x_cur": jax.random.normal(part_keys[1], (GRID_NODES, VARS), jnp.float32),
        "forcing": jax.random.normal(part_keys[2], (GRID_NODES, 2, FORCE), jnp.float32),
        "grid_static": jax.random.normal(part_keys[3], (GRID_NODES, STATIC), jnp.float32),
        "g2m_feat": jax.random.normal(part_keys[4], (GRID_NODES, EDGE_FEAT), jnp.float32),
        "m2g_feat": jax.random.normal(part_keys[5], (GRID_NODES, EDGE_FEAT), jnp.float32),
        "mesh_feat": jax.random.normal(part_keys[6], (MESH_NODES, MESH_FEAT), jnp.float32),
        "mesh_edge_feat": jax.random.normal(part_keys[7], (MESH_NODES, OFFSET_COUNT, EDGE_FEAT), jnp.float32),
        "norm_stats": norm_stats,
        "w_grid_in": normal_weight(weight_keys[4], (IN_FEAT, LATENT), IN_FEAT),
        "w_mesh_in": normal_weight(weight_keys[5], (MESH_FEAT, LATENT), MESH_FEAT),
        "w_eemb_in": normal_weight(weight_keys[6], (3, EDGE_FEAT, LATENT), EDGE_FEAT),
        "w_embed_out": normal_weight(weight_keys[7], (5, LATENT, LATENT), LATENT),
        "w_edge_in": normal_weight(weight_keys[8], (BLOCKS, 3 * LATENT, LATENT), 3 * LATENT),
        "w_edge_out": normal_weight(weight_keys[9], (BLOCKS, LATENT, LATENT), LATENT),
        "w_node_in": normal_weight(weight_keys[10], (BLOCKS, 2 * LATENT, LATENT), 2 * LATENT),
        "w_node_out": normal_weight(weight_keys[11], (BLOCKS, LATENT, LATENT), LATENT),
        "w_grid_self": normal_weight(weight_keys[12], (2, LATENT, LATENT), LATENT),
        "w_out_hidden": normal_weight(weight_keys[13], (LATENT, LATENT), LATENT),
        "w_out_final": normal_weight(weight_keys[14], (LATENT, VARS), LATENT),
    }


def layer_norm(values):
    centre = jnp.mean(values, axis=-1, keepdims=True)
    centred = values - centre
    spread = jnp.mean(centred * centred, axis=-1, keepdims=True)
    return centred * lax.rsqrt(spread + 1e-5)


def matmul_f32(values, weight):
    return jnp.dot(values, weight, preferred_element_type=jnp.float32)


def mlp_tail(pre_act, w_second):
    hidden = jax.nn.silu(pre_act).astype(jnp.bfloat16)
    return layer_norm(matmul_f32(hidden, w_second))


def residual(base, update):
    return (base.astype(jnp.float32) + update).astype(jnp.bfloat16)


def embed_static(features, w_first, w_second):
    return mlp_tail(matmul_f32(features.astype(jnp.bfloat16), w_first), w_second).astype(jnp.bfloat16)


def reference(x_prev, x_cur, forcing, grid_static, g2m_feat, m2g_feat, mesh_feat, mesh_edge_feat, norm_stats, w_grid_in, w_mesh_in, w_eemb_in, w_embed_out, w_edge_in, w_edge_out, w_node_in, w_node_out, w_grid_self, w_out_hidden, w_out_final):
    mesh_lat = embed_static(mesh_feat, w_mesh_in, w_embed_out[1])
    g2m_lat = embed_static(g2m_feat, w_eemb_in[0], w_embed_out[2])
    m2g_lat = embed_static(m2g_feat, w_eemb_in[1], w_embed_out[3])
    edge_base = embed_static(mesh_edge_feat.reshape(MESH_NODES * OFFSET_COUNT, EDGE_FEAT), w_eemb_in[2], w_embed_out[4])
    in_mean = norm_stats[0]
    in_std = norm_stats[1]
    diff_mean = norm_stats[2]
    diff_std = norm_stats[3]

    def proc_layer(layer_state, layer_weights):
        mesh_cur, edge_lat = layer_state
        w_edge, w_edge_two, w_node, w_node_two = layer_weights
        send_proj = matmul_f32(mesh_cur, w_edge[LATENT:2 * LATENT])
        send_term = jnp.stack([jnp.roll(send_proj, -offset, axis=0) for offset in OFFSETS], axis=1).reshape(MESH_NODES * OFFSET_COUNT, LATENT)
        recv_term = matmul_f32(mesh_cur, w_edge[2 * LATENT:])
        pre_act = matmul_f32(edge_lat, w_edge[:LATENT]) + send_term
        pre_act = (pre_act.reshape(MESH_NODES, OFFSET_COUNT, LATENT) + recv_term[:, None, :]).reshape(MESH_NODES * OFFSET_COUNT, LATENT)
        edge_lat = residual(edge_lat, mlp_tail(pre_act, w_edge_two))
        edge_sum = jnp.sum(edge_lat.reshape(MESH_NODES, OFFSET_COUNT, LATENT).astype(jnp.float32), axis=1).astype(jnp.bfloat16)
        mesh_cur = residual(mesh_cur, mlp_tail(matmul_f32(mesh_cur, w_node[:LATENT]) + matmul_f32(edge_sum, w_node[LATENT:]), w_node_two))
        return (mesh_cur, edge_lat), None

    def forecast_step(state_pair, force_now):
        state_prev, state_cur = state_pair
        features = jnp.concatenate([(state_prev - in_mean) / in_std, (state_cur - in_mean) / in_std, force_now, grid_static], axis=1)
        grid_lat = embed_static(features, w_grid_in, w_embed_out[0])
        w_first = w_edge_in[0]
        senders = jnp.roll(grid_lat, SHIFT * GRID_RATIO, axis=0)
        recv_term = matmul_f32(mesh_lat, w_first[2 * LATENT:])
        pre_act = matmul_f32(g2m_lat, w_first[:LATENT]) + matmul_f32(senders, w_first[LATENT:2 * LATENT])
        pre_act = (pre_act.reshape(MESH_NODES, GRID_RATIO, LATENT) + recv_term[:, None, :]).reshape(GRID_NODES, LATENT)
        enc_edge = residual(g2m_lat, mlp_tail(pre_act, w_edge_out[0]))
        enc_sum = jnp.sum(enc_edge.reshape(MESH_NODES, GRID_RATIO, LATENT).astype(jnp.float32), axis=1).astype(jnp.bfloat16)
        node_first = w_node_in[0]
        mesh_cur = residual(mesh_lat, mlp_tail(matmul_f32(mesh_lat, node_first[:LATENT]) + matmul_f32(enc_sum, node_first[LATENT:]), w_node_out[0]))
        grid_cur = residual(grid_lat, mlp_tail(matmul_f32(grid_lat, w_grid_self[0]), w_grid_self[1]))
        layer_weights = (w_edge_in[1:BLOCKS - 1], w_edge_out[1:BLOCKS - 1], w_node_in[1:BLOCKS - 1], w_node_out[1:BLOCKS - 1])
        layer_out, no_stack = lax.scan(proc_layer, (mesh_cur, edge_base), layer_weights)
        mesh_cur = layer_out[0]
        w_last = w_edge_in[BLOCKS - 1]
        send_term = matmul_f32(jnp.roll(mesh_cur, -SHIFT, axis=0), w_last[LATENT:2 * LATENT])
        pre_act = matmul_f32(m2g_lat, w_last[:LATENT]) + matmul_f32(grid_cur, w_last[2 * LATENT:])
        pre_act = (pre_act.reshape(MESH_NODES, GRID_RATIO, LATENT) + send_term[:, None, :]).reshape(GRID_NODES, LATENT)
        dec_edge = residual(m2g_lat, mlp_tail(pre_act, w_edge_out[BLOCKS - 1]))
        node_last = w_node_in[BLOCKS - 1]
        grid_out = residual(grid_cur, mlp_tail(matmul_f32(grid_cur, node_last[:LATENT]) + matmul_f32(dec_edge, node_last[LATENT:]), w_node_out[BLOCKS - 1]))
        hidden = jax.nn.silu(matmul_f32(grid_out, w_out_hidden)).astype(jnp.bfloat16)
        prediction = matmul_f32(hidden, w_out_final)
        state_next = state_cur + diff_std * prediction + diff_mean
        return (state_cur, state_next), state_next

    final_pair, stacked = lax.scan(forecast_step, (x_prev, x_cur), jnp.swapaxes(forcing, 0, 1))
    return stacked[0], stacked[1]
```

```python
import jax
import jax.numpy as jnp
import numpy as np
from jax import lax
from jax.experimental import pallas as pl
from jax.experimental.pallas import tpu as pltpu
from jax.sharding import PartitionSpec as P

MESH_ID = pl.DeviceIdType.MESH
F32 = jnp.float32
BF16 = jnp.bfloat16
SUB = 256


def dot(a, b):
    return jnp.dot(a, b, preferred_element_type=F32)


def silu(x):
    half = 0.5 * x
    return (half * jnp.tanh(half) + half).astype(BF16)


def norm(y):
    z = y - jnp.mean(y, axis=-1, keepdims=True)
    return z * lax.rsqrt(jnp.mean(z * z, axis=-1, keepdims=True) + 1e-5)


def residual(base, update):
    return (base.astype(F32) + update).astype(BF16)


def row_permutation():
    perm = np.zeros((256, 256), np.float32)
    for r in range(4):
        for j in range(8):
            for i in range(8):
                perm[r * 64 + j * 8 + i, (i * 8 + j) * 4 + r] = 1.0
    return np.stack([perm, perm.T])


def solution(mesh):
    group = mesh.shape["gp"]

    def kernel(f0, xc_hbm, ef_hbm, mf, stats, perms, wg, wemb, wembo, wei_hbm, weo_hbm, wni_hbm, wno_hbm, wgs, woh, wof,
               out0, out1,
               wei, weo, wni, wno, xst, xs, fm, g2m, m2g, glat, gcur, mlat, efl, ebase, elat, hsend, hin, hcur, hd,
               proj, recv, halo_s, halo_r, stage,
               wsem, xsem, osem, ef_s, ef_r, en_s, en_r, de_s, de_r, ha_s, ha_r):
        me = lax.axis_index("gp")
        left = lax.rem(me + group - 1, group)
        right = lax.rem(me + 1, group)
        blocks = 2 * group
        layers = wei_hbm.shape[0]

        barrier = pltpu.get_barrier_semaphore()
        for hop in range(1, group):
            pl.semaphore_signal(barrier, inc=1, device_id={"gp": lax.rem(me + hop, group)}, device_id_type=MESH_ID)

        weight_copies = [pltpu.make_async_copy(src, dst, wsem.at[i]) for i, (src, dst) in enumerate(
            [(wei_hbm, wei), (weo_hbm, weo), (wni_hbm, wni), (wno_hbm, wno)])]
        x_copy = pltpu.make_async_copy(xc_hbm, xst.at[0], xsem)
        x_copy.start()
        for copy in weight_copies:
            copy.start()
        pl.semaphore_wait(barrier, group - 1)

        def block_of(device, half):
            return lax.rem(2 * device + half, blocks)

        def ef_copy(hop, half):
            dest = lax.rem(me + hop, group)
            return pltpu.make_async_remote_copy(
                src_ref=ef_hbm.at[half, dest], dst_ref=efl.at[2 * me + half], send_sem=ef_s.at[dest, half],
                recv_sem=ef_r.at[me, half], device_id={"gp": dest}, device_id_type=MESH_ID)

        def ef_keep(half):
            return pltpu.make_async_copy(ef_hbm.at[half, me], efl.at[2 * me + half], ef_r.at[me, half])

        for half in range(2):
            for hop in range(1, group):
                ef_copy(hop, half).start()
            ef_keep(half).start()

        def embed_rows(it, carry):
            for sub in range(4):
                base = pl.multiple_of((it * 4 + sub) * 256, 256)
                rows = pl.ds(base, 256)
                feats = dot(perms[0], f0[rows, :]).astype(BF16)
                xs[0, rows, :] = feats[:, 0:128]
                xs[1, rows, :] = feats[:, 128:256]
                misc = feats[:, 256:384]
                fm[rows, :] = misc
                g2m[rows, :] = norm(dot(silu(dot(misc, wemb[0])), wembo[2])).astype(BF16)
                m2g[rows, :] = norm(dot(silu(dot(misc, wemb[1])), wembo[3])).astype(BF16)
            return carry

        lax.fori_loop(0, 4, embed_rows, 0)
        for sub in range(4):
            rows = pl.ds(sub * 256, 256)
            mlat[rows, :] = norm(dot(silu(dot(mf[rows, :], wemb[2])), wembo[1])).astype(BF16)
        xs[2] = jnp.zeros(xs.shape[1:], BF16)
        for copy in weight_copies:
            copy.wait()

        def en_copy(hop, half):
            dest = lax.rem(me + hop, group)
            return pltpu.make_async_remote_copy(
                src_ref=hsend.at[half, dest], dst_ref=hin.at[block_of(me, 1 + half)], send_sem=en_s.at[dest, half],
                recv_sem=en_r.at[me, half], device_id={"gp": dest}, device_id_type=MESH_ID)

        def de_copy(hop, half):
            dest = lax.rem(me + hop, group)
            return pltpu.make_async_remote_copy(
                src_ref=hcur.at[block_of(dest, 1 + half)], dst_ref=hd.at[half, me], send_sem=de_s.at[dest, half],
                recv_sem=de_r.at[me, half], device_id={"gp": dest}, device_id_type=MESH_ID)

        def en_arrival(source, half):
            return pltpu.make_async_remote_copy(
                src_ref=hsend.at[half, me], dst_ref=hin.at[block_of(source, 1 + half)], send_sem=en_s.at[me, half],
                recv_sem=en_r.at[source, half], device_id={"gp": left}, device_id_type=MESH_ID)

        def de_arrival(source, half):
            return pltpu.make_async_remote_copy(
                src_ref=hcur.at[0], dst_ref=hd.at[half, source], send_sem=de_s.at[me, half],
                recv_sem=de_r.at[source, half], device_id={"gp": left}, device_id_type=MESH_ID)

        def ef_arrival(source, half):
            return pltpu.make_async_remote_copy(
                src_ref=ef_hbm.at[half, me], dst_ref=efl.at[2 * source + half], send_sem=ef_s.at[me, half],
                recv_sem=ef_r.at[source, half], device_id={"gp": left}, device_id_type=MESH_ID)

        def halo_copies(slot):
            return [pltpu.make_async_remote_copy(
                src_ref=halo_s.at[slot, side], dst_ref=halo_r.at[slot, 1 - side], send_sem=ha_s.at[slot, side],
                recv_sem=ha_r.at[slot, 1 - side], device_id={"gp": (left, right)[side]}, device_id_type=MESH_ID)
                for side in range(2)]

        def send_halo(slot):
            for b in range(blocks):
                stage[0, b:b + 1, :] = hcur[b, 0:16, :].astype(F32)[0:1]
                stage[1, b:b + 1, :] = hcur[b, 48:64, :].astype(F32)[15:16]
            halo_s[slot, 0] = stage[0].astype(BF16)
            halo_s[slot, 1] = stage[1].astype(BF16)
            for copy in halo_copies(slot):
                copy.start()

        def rolled(shift):
            cut = shift % blocks
            return jnp.concatenate([proj[cut:, 8:72, :], proj[:cut, 8:72, :]], axis=0)

        def edge_update(layer, k, send):
            send = send.reshape(blocks * 64, 256)
            w_first = wei[layer, 0:256, :]
            w_second = weo[layer]
            for sub in range(0, blocks * 64, SUB):
                rows = slice(sub, sub + SUB)
                old = elat[k, rows, :]
                pre = dot(old, w_first) + (send[rows] + recv[rows, :])
                elat[k, rows, :] = residual(old, norm(dot(silu(pre), w_second)))

        def mesh_layer(layer, carry):
            slot = lax.rem(layer, 2)
            h = hcur[...].reshape(blocks * 64, 256)
            proj[:, 8:72, :] = dot(h, wei[layer, 256:512, :]).reshape(blocks, 64, 256)
            recv[...] = dot(h, wei[layer, 512:768, :])
            for k, shift in ((2, 1), (3, -1), (4, 4), (5, -4)):
                edge_update(layer, k, rolled(shift))
            for copy in halo_copies(slot):
                copy.wait_recv()
            for copy in halo_copies(slot):
                copy.wait_send()
            edge_proj = dot(halo_r[slot].reshape(32, 256), wei[layer, 256:512, :])
            low = edge_proj[0:16]
            high = edge_proj[16:32]
            stage[0] = jnp.where(me == 0, jnp.concatenate([low[15:16], low[0:15]], axis=0), low)
            stage[1] = jnp.where(me == group - 1, jnp.concatenate([high[1:16], high[0:1]], axis=0), high)
            sublane = lax.broadcasted_iota(jnp.int32, (8, 256), 0)
            for b in range(blocks):
                proj[b, 0:8, :] = jnp.where(sublane == 0, stage[0, b:b + 1, :], pltpu.roll(proj[b, 64:72, :], 1, 0))
                proj[b, 72:80, :] = jnp.where(sublane == 7, stage[1, b:b + 1, :], pltpu.roll(proj[b, 8:16, :], 7, 0))
            edge_update(layer, 0, proj[:, 16:80, :])
            edge_update(layer, 1, proj[:, 0:64, :])
            for sub in range(0, blocks, SUB // 64):
                node = hcur[sub:sub + SUB // 64].reshape(SUB, 256)
                rows = slice(sub * 64, sub * 64 + SUB)
                total = elat[0, rows, :].astype(F32)
                for k in range(1, 6):
                    total = total + elat[k, rows, :].astype(F32)
                pre = dot(node, wni[layer, 0:256, :]) + dot(total.astype(BF16), wni[layer, 256:512, :])
                new = residual(node, norm(dot(silu(pre), wno[layer])))
                hcur[sub:sub + SUB // 64] = new.reshape(SUB // 64, 64, 256)

            @pl.when(layer < layers - 2)
            def _():
                send_halo(1 - slot)
            return carry

        def forecast(step, carry):
            def encode(it, carry):
                for q in range(2):
                    hop = 2 * it + 1 + q
                    dest = lax.rem(me + hop, group)
                    esums = []
                    nodes = []
                    for half in range(2):
                        chunk = half * group + dest
                        rows = pl.ds(pl.multiple_of(chunk * 256, 256), 256)
                        mrows = pl.ds(pl.multiple_of(chunk * 64, 64), 64)
                        feats = jnp.concatenate([xs[step, rows, :], xs[step + 1, rows, :]], axis=1)
                        pre = dot(feats, wg[step, 0:256, :]) + dot(fm[rows, :], wg[step, 256:384, :])
                        lat = norm(dot(silu(pre), wembo[0])).astype(BF16)
                        glat[rows, :] = lat
                        node = mlat[mrows, :]
                        term = dot(node, wei[0, 512:768, :])
                        old = g2m[rows, :]
                        pre = dot(old, wei[0, 0:256, :]) + dot(lat, wei[0, 256:512, :])
                        pre = pre + jnp.concatenate([term] * 4, axis=0)
                        edge = residual(old, norm(dot(silu(pre), weo[0]))).astype(F32)
                        esums.append((edge[0:64] + edge[64:128] + edge[128:192] + edge[192:256]).astype(BF16))
                        nodes.append(node)
                    node = jnp.concatenate(nodes, axis=0)
                    pre = dot(node, wni[0, 0:256, :]) + dot(jnp.concatenate(esums, axis=0), wni[0, 256:512, :])
                    new = residual(node, norm(dot(silu(pre), wno[0])))
                    for half in range(2):
                        hsend[half, dest] = new[half * 64:half * 64 + 64]
                for half in range(2):
                    en_copy(2 * it + 1, half).start()

                @pl.when(it < group // 2 - 1)
                def _():
                    for half in range(2):
                        en_copy(2 * it + 2, half).start()
                return carry

            lax.fori_loop(0, group // 2, encode, 0)

            @pl.when(step == 0)
            def _():
                for half in range(2):
                    for hop in range(1, group):
                        ef_arrival(lax.rem(me + hop, group), half).wait_recv()
                    ef_keep(half).wait()

                def embed_edges(k, carry):
                    for sub in range(0, blocks, 4):
                        feats = efl[sub:sub + 4].reshape(256, 128)
                        ebase[k, sub * 64:sub * 64 + 256, :] = norm(dot(silu(dot(feats, wemb[3 + k])), wembo[4])).astype(BF16)
                    return carry

                lax.fori_loop(0, 6, embed_edges, 0)
                for hop in range(1, group):
                    for half in range(2):
                        ef_copy(hop, half).wait_send()

            elat[...] = ebase[...]
            for hop in range(1, group):
                for half in range(2):
                    en_arrival(lax.rem(me + hop, group), half).wait_recv()
            for hop in range(1, group):
                for half in range(2):
                    en_copy(hop, half).wait_send()
            hcur[...] = hin[...]
            for half in range(2):
                hcur[block_of(me, 1 + half)] = hsend[half, me]
            send_halo(1)
            lax.fori_loop(1, layers - 1, mesh_layer, 0)
            for hop in range(1, group):
                for half in range(2):
                    de_copy(hop, half).start()
            for half in range(2):
                hd[half, me] = hcur[block_of(me, 1 + half)]

            def self_update(it, carry):
                for sub in range(4):
                    rows = pl.ds(pl.multiple_of((it * 4 + sub) * 256, 256), 256)
                    old = glat[rows, :]
                    gcur[rows, :] = residual(old, norm(dot(silu(dot(old, wgs[0])), wgs[1])))
                return carry

            lax.fori_loop(0, 4, self_update, 0)

            @pl.when(step == 0)
            def _():
                x_copy.wait()

            def decode(it, carry):
                last = layers - 1
                for half in range(2):
                    de_arrival(lax.rem(me + 2 * it + 1, group), half).wait_recv()

                @pl.when(it < group // 2 - 1)
                def _():
                    for half in range(2):
                        de_arrival(lax.rem(me + 2 * it + 2, group), half).wait_recv()

                work = []
                for q in range(2):
                    source = lax.rem(me + 2 * it + 1 + q, group)
                    for half in range(2):
                        rows = pl.ds(pl.multiple_of((half * group + source) * 256, 256), 256)
                        work.append((rows, hd[half, source], m2g[rows, :], gcur[rows, :], xst[step, rows, :]))
                done = []
                for rows, node, old, grid, state in work:
                    term = dot(node, wei[last, 256:512, :])
                    pre = dot(old, wei[last, 0:256, :]) + dot(grid, wei[last, 512:768, :])
                    pre = pre + jnp.concatenate([term] * 4, axis=0)
                    edge = residual(old, norm(dot(silu(pre), weo[last])))
                    pre = dot(grid, wni[last, 0:256, :]) + dot(edge, wni[last, 256:512, :])
                    out = residual(grid, norm(dot(silu(pre), wno[last])))
                    hidden = silu(dot(out, woh[...]))
                    hidden = dot(perms[1], hidden).astype(BF16)
                    new = state + stats[3:4, :] * dot(hidden, wof[...]) + stats[2:3, :]
                    scaled = ((new - stats[0:1, :]) / stats[1:2, :]).astype(BF16)
                    done.append((rows, new, dot(perms[0], scaled).astype(BF16)))
                for rows, new, scaled in done:
                    xst[step + 1, rows, :] = new
                    xs[2, rows, 0:scaled.shape[1]] = scaled
                return carry

            lax.fori_loop(0, group // 2, decode, 0)
            for hop in range(1, group):
                for half in range(2):
                    de_copy(hop, half).wait_send()

            @pl.when(step == 0)
            def _():
                pltpu.make_async_copy(xst.at[1], out0, osem.at[0]).start()
            return carry

        lax.fori_loop(0, 2, forecast, 0)
        final = pltpu.make_async_copy(xst.at[2], out1, osem.at[1])
        final.start()
        pltpu.make_async_copy(xst.at[1], out0, osem.at[0]).wait()
        final.wait()

    def shift_pairs(hop_count):
        return [(source, (source + hop_count) % group) for source in range(group)]

    def local_run(x_prev, x_cur, forcing, grid_static, g2m_feat, m2g_feat, mesh_feat, mesh_edge_feat, norm_stats, w_grid_in, w_mesh_in, w_eemb_in, w_embed_out, w_edge_in, w_edge_out, w_node_in, w_node_out, w_grid_self, w_out_hidden, w_out_final):
        grid_dev, variables = x_prev.shape
        mesh_dev = mesh_feat.shape[0]
        latent = w_embed_out.shape[-1]
        blocks = 2 * group
        half_grid = grid_dev // 2
        half_mesh = mesh_dev // 2

        def shifted(values, half):
            head = lax.ppermute(values[:half], "gp", shift_pairs(-1))
            return jnp.concatenate([values[half:], head], axis=0)

        def in_order(values):
            lanes = values.shape[-1]
            values = values.reshape(2, group, 8, 8, lanes).transpose(0, 1, 3, 2, 4)
            return values.reshape(2, group, 64, lanes)

        def lane_pad(values, width):
            return jnp.pad(values, [(0, 0)] * (values.ndim - 1) + [(0, width - values.shape[-1])])

        g2m_here = shifted(g2m_feat, half_grid)
        mesh_here = shifted(mesh_feat, half_mesh)
        misc = jnp.concatenate([forcing[:, 0, :], forcing[:, 1, :], grid_static, g2m_here, m2g_feat], axis=1)
        force = forcing.shape[-1]
        static = grid_static.shape[-1]
        edge_lanes = g2m_feat.shape[-1]
        scale = lambda x: (x - norm_stats[0]) / norm_stats[1]
        feats = jnp.concatenate([lane_pad(scale(x_prev), 128), lane_pad(scale(x_cur), 128), lane_pad(misc, 128)], axis=1).astype(BF16)
        mesh_rows = lane_pad(in_order(mesh_here).astype(BF16), 128).reshape(mesh_dev, 128)
        edge_rows = lane_pad(in_order(mesh_edge_feat.reshape(mesh_dev, -1)).astype(BF16), 128)

        def placed(rows, start, height):
            return jnp.pad(rows, ((start, height - start - rows.shape[0]), (0, 0)))

        w_force = w_grid_in[2 * variables:2 * variables + force]
        w_static = w_grid_in[2 * variables + force:]
        w_state = placed(w_grid_in[:variables], 0, 384) + placed(w_grid_in[variables:2 * variables], 128, 384) + placed(w_static, 256 + 2 * force, 384)
        w_grid = jnp.stack([w_state + placed(w_force, 256 + force * s, 384) for s in range(2)])
        at_g2m = 2 * force + static
        w_embed = jnp.stack([placed(w_eemb_in[0], at_g2m, 128), placed(w_eemb_in[1], at_g2m + edge_lanes, 128), placed(w_mesh_in, 0, 128)]
                            + [placed(w_eemb_in[2], edge_lanes * k, 128) for k in range(6)])
        perms = jnp.asarray(row_permutation(), BF16)

        vmem = pl.BlockSpec(memory_space=pltpu.VMEM)
        anywhere = pl.BlockSpec(memory_space=pl.ANY)
        state = jax.ShapeDtypeStruct((grid_dev, variables), F32)
        dma = pltpu.SemaphoreType.DMA
        return pl.pallas_call(
            kernel,
            out_shape=(state, state),
            in_specs=[vmem, anywhere, anywhere] + [vmem] * 6 + [anywhere] * 4 + [vmem] * 3,
            out_specs=(anywhere, anywhere),
            scratch_shapes=[
                pltpu.VMEM(w_edge_in.shape, BF16), pltpu.VMEM(w_edge_out.shape, BF16),
                pltpu.VMEM(w_node_in.shape, BF16), pltpu.VMEM(w_node_out.shape, BF16),
                pltpu.VMEM((3, grid_dev, variables), F32), pltpu.VMEM((3, grid_dev, 128), BF16), pltpu.VMEM((grid_dev, 128), BF16),
                pltpu.VMEM((grid_dev, latent), BF16), pltpu.VMEM((grid_dev, latent), BF16), pltpu.VMEM((grid_dev, latent), BF16),
                pltpu.VMEM((grid_dev, latent), BF16),
                pltpu.VMEM((mesh_dev, latent), BF16), pltpu.VMEM((blocks, 64, 128), BF16),
                pltpu.VMEM((6, mesh_dev, latent), BF16), pltpu.VMEM((6, mesh_dev, latent), BF16),
                pltpu.VMEM((2, group, 64, latent), BF16), pltpu.VMEM((blocks, 64, latent), BF16),
                pltpu.VMEM((blocks, 64, latent), BF16), pltpu.VMEM((2, group, 64, latent), BF16),
                pltpu.VMEM((blocks, 80, latent), F32), pltpu.VMEM((mesh_dev, latent), F32),
                pltpu.VMEM((2, 2, blocks, latent), BF16), pltpu.VMEM((2, 2, blocks, latent), BF16), pltpu.VMEM((2, blocks, latent), F32),
                dma((4,)), dma, dma((2,)), dma((group, 2)), dma((group, 2)), dma((group, 2)), dma((group, 2)),
                dma((group, 2)), dma((group, 2)), dma((2, 2)), dma((2, 2)),
            ],
            compiler_params=pltpu.CompilerParams(collective_id=0, has_side_effects=True, vmem_limit_bytes=67043328),
        )(feats, x_cur, edge_rows, mesh_rows, norm_stats, perms, w_grid, w_embed, w_embed_out, w_edge_in, w_edge_out, w_node_in, w_node_out,
          w_grid_self, w_out_hidden, w_out_final)

    row_spec = P(("dp", "gp"))
    edge_spec = P(("dp", "gp"), None, None)
    whole = P()
    in_specs = (row_spec, row_spec, edge_spec, row_spec, row_spec, row_spec, row_spec, edge_spec, whole) + (whole,) * 11
    return jax.shard_map(local_run, mesh=mesh, in_specs=in_specs, out_specs=(row_spec, row_spec), check_vma=False)
```

```python
import jax
import jax.numpy as jnp
import numpy as np
from jax import lax
from jax.experimental import pallas as pl
from jax.experimental.pallas import tpu as pltpu
from jax.sharding import PartitionSpec as P

MESH_ID = pl.DeviceIdType.MESH
F32 = jnp.float32
BF16 = jnp.bfloat16
SUB = 256
PER = 4
RECV_MXU = False
SUM_MXU = False
FLAGS = {}


def dot(a, b):
    return jnp.dot(a, b, preferred_element_type=F32)


def silu_of_half(half):
    return (half * jnp.tanh(half) + half).astype(BF16)


def norm(y):
    z = y - jnp.mean(y, axis=-1, keepdims=True)
    return z * lax.rsqrt(jnp.mean(z * z, axis=-1, keepdims=True) + 1e-5)


def residual(base, update):
    return (base.astype(F32) + update).astype(BF16)


def row_permutation():
    perm = np.zeros((256, 256), np.float32)
    for r in range(4):
        for j in range(8):
            for i in range(8):
                perm[r * 64 + j * 8 + i, (i * 8 + j) * 4 + r] = 1.0
    return np.stack([perm, perm.T, np.eye(256, dtype=np.float32)])


def solution(mesh):
    group = mesh.shape["gp"]

    def kernel(f0, xc_hbm, ef_hbm, mf, stats, perms, wg, wemb, wembo, wei_hbm, weo_hbm, wni_hbm, wno_hbm, wgs, woh, wof,
               out0, out1,
               wei, weo, wni, wno, xst, xs, fm, g2m, m2g, glat, gcur, mlat, efl, ebase, elat, hsend, hin, hcur, hd,
               proj, recv, halo_s, halo_r, stage, wsh,
               wsem, xsem, osem, ef_s, ef_r, en_s, en_r, de_s, de_r, ha_s, ha_r):
        me = lax.axis_index("gp")
        left = lax.rem(me + group - 1, group)
        right = lax.rem(me + 1, group)
        blocks = 2 * group
        layers = wei_hbm.shape[0]

        barrier = pltpu.get_barrier_semaphore()
        for hop in range(1, group):
            pl.semaphore_signal(barrier, inc=1, device_id={"gp": lax.rem(me + hop, group)}, device_id_type=MESH_ID)

        weight_copies = [pltpu.make_async_copy(src, dst, wsem.at[i]) for i, (src, dst) in enumerate(
            [(wei_hbm, wei), (weo_hbm, weo), (wni_hbm, wni), (wno_hbm, wno)])]
        x_copy = pltpu.make_async_copy(xc_hbm, xst.at[0], xsem)
        x_copy.start()
        for copy in weight_copies:
            copy.start()
        pl.semaphore_wait(barrier, group - 1)

        def block_of(device, half):
            return lax.rem(2 * device + half, blocks)

        def ef_copy(hop, half):
            dest = lax.rem(me + hop, group)
            return pltpu.make_async_remote_copy(
                src_ref=ef_hbm.at[half, dest], dst_ref=efl.at[2 * me + half], send_sem=ef_s.at[dest, half],
                recv_sem=ef_r.at[me, half], device_id={"gp": dest}, device_id_type=MESH_ID)

        def ef_keep(half):
            return pltpu.make_async_copy(ef_hbm.at[half, me], efl.at[2 * me + half], ef_r.at[me, half])

        for half in range(2):
            for hop in range(1, group):
                ef_copy(hop, half).start()
            ef_keep(half).start()

        def embed_rows(it, carry):
            for sub in range(4):
                base = pl.multiple_of((it * 4 + sub) * 256, 256)
                rows = pl.ds(base, 256)
                feats = dot(perms[0], f0[rows, :]).astype(BF16)
                xs[0, rows, :] = feats[:, 0:128]
                xs[1, rows, :] = feats[:, 128:256]
                misc = feats[:, 256:384]
                fm[rows, :] = misc
                g2m[rows, :] = norm(dot(silu_of_half(dot(misc, wemb[0])), wembo[2])).astype(BF16)
                m2g[rows, :] = norm(dot(silu_of_half(dot(misc, wemb[1])), wembo[3])).astype(BF16)
            return carry

        lax.fori_loop(0, 4, embed_rows, 0)
        for sub in range(4):
            rows = pl.ds(sub * 256, 256)
            mlat[rows, :] = norm(dot(silu_of_half(dot(mf[rows, :], wemb[2])), wembo[1])).astype(BF16)
        xs[2] = jnp.zeros(xs.shape[1:], BF16)
        for copy in weight_copies:
            copy.wait()

        def halve(layer, carry):
            wei[layer] = wei[layer] * 0.5
            wni[layer] = wni[layer] * 0.5
            return carry

        lax.fori_loop(0, layers, halve, 0)
        wsh[0] = wgs[0] * 0.5
        wsh[1] = woh[...] * 0.5

        def en_copy(hop, half):
            dest = lax.rem(me + hop, group)
            return pltpu.make_async_remote_copy(
                src_ref=hsend.at[half, dest], dst_ref=hin.at[block_of(me, 1 + half)], send_sem=en_s.at[dest, half],
                recv_sem=en_r.at[me, half], device_id={"gp": dest}, device_id_type=MESH_ID)

        def de_copy(hop, half):
            dest = lax.rem(me + hop, group)
            return pltpu.make_async_remote_copy(
                src_ref=hcur.at[block_of(dest, 1 + half)], dst_ref=hd.at[half, me], send_sem=de_s.at[dest, half],
                recv_sem=de_r.at[me, half], device_id={"gp": dest}, device_id_type=MESH_ID)

        def en_arrival(source, half):
            return pltpu.make_async_remote_copy(
                src_ref=hsend.at[half, me], dst_ref=hin.at[block_of(source, 1 + half)], send_sem=en_s.at[me, half],
                recv_sem=en_r.at[source, half], device_id={"gp": left}, device_id_type=MESH_ID)

        def de_arrival(source, half):
            return pltpu.make_async_remote_copy(
                src_ref=hcur.at[0], dst_ref=hd.at[half, source], send_sem=de_s.at[me, half],
                recv_sem=de_r.at[source, half], device_id={"gp": left}, device_id_type=MESH_ID)

        def ef_arrival(source, half):
            return pltpu.make_async_remote_copy(
                src_ref=ef_hbm.at[half, me], dst_ref=efl.at[2 * source + half], send_sem=ef_s.at[me, half],
                recv_sem=ef_r.at[source, half], device_id={"gp": left}, device_id_type=MESH_ID)

        def halo_copies(slot):
            return [pltpu.make_async_remote_copy(
                src_ref=halo_s.at[slot, side], dst_ref=halo_r.at[slot, 1 - side], send_sem=ha_s.at[slot, side],
                recv_sem=ha_r.at[slot, 1 - side], device_id={"gp": (left, right)[side]}, device_id_type=MESH_ID)
                for side in range(2)]

        def send_halo(slot):
            for b in range(blocks):
                stage[0, b:b + 1, :] = hcur[b, 0:16, :].astype(F32)[0:1]
                stage[1, b:b + 1, :] = hcur[b, 48:64, :].astype(F32)[15:16]
            halo_s[slot, 0] = stage[0].astype(BF16)
            halo_s[slot, 1] = stage[1].astype(BF16)
            for copy in halo_copies(slot):
                copy.start()

        def rolled(shift):
            cut = shift % blocks
            return jnp.concatenate([proj[cut:, 8:72, :], proj[:cut, 8:72, :]], axis=0)

        def edge_update(layer, k, send):
            send = send.reshape(blocks * 64, 256)
            w_first = wei[layer, 0:256, :]
            w_second = weo[layer]
            for sub in range(0, blocks * 64, SUB):
                rows = slice(sub, sub + SUB)
                old = elat[k, rows, :]
                if RECV_MXU:
                    node = hcur[sub // 64:(sub + SUB) // 64].reshape(SUB, 256)
                    pre = dot(jnp.concatenate([old, node], axis=1), jnp.concatenate([w_first, wei[layer, 512:768, :]], axis=0)) + send[rows]
                else:
                    pre = dot(old, w_first) + (send[rows] + recv[rows, :])
                elat[k, rows, :] = residual(old, norm(dot(silu_of_half(pre), w_second)))

        def mesh_layer(layer, carry):
            slot = lax.rem(layer, 2)
            h = hcur[...].reshape(blocks * 64, 256)
            proj[:, 8:72, :] = dot(h, wei[layer, 256:512, :]).reshape(blocks, 64, 256)
            if not RECV_MXU:
                recv[...] = dot(h, wei[layer, 512:768, :])
            for k, shift in ((2, 1), (3, -1), (4, 4), (5, -4)):
                edge_update(layer, k, rolled(shift))
            for copy in halo_copies(slot):
                copy.wait_recv()
            for copy in halo_copies(slot):
                copy.wait_send()
            edge_proj = dot(halo_r[slot].reshape(32, 256), wei[layer, 256:512, :])
            low = edge_proj[0:16]
            high = edge_proj[16:32]
            stage[0] = jnp.where(me == 0, jnp.concatenate([low[15:16], low[0:15]], axis=0), low)
            stage[1] = jnp.where(me == group - 1, jnp.concatenate([high[1:16], high[0:1]], axis=0), high)
            sublane = lax.broadcasted_iota(jnp.int32, (8, 256), 0)
            for b in range(blocks):
                proj[b, 0:8, :] = jnp.where(sublane == 0, stage[0, b:b + 1, :], pltpu.roll(proj[b, 64:72, :], 1, 0))
                proj[b, 72:80, :] = jnp.where(sublane == 7, stage[1, b:b + 1, :], pltpu.roll(proj[b, 8:16, :], 7, 0))
            edge_update(layer, 0, proj[:, 16:80, :])
            edge_update(layer, 1, proj[:, 0:64, :])
            for sub in range(0, blocks, SUB // 64):
                node = hcur[sub:sub + SUB // 64].reshape(SUB, 256)
                rows = slice(sub * 64, sub * 64 + SUB)
                if SUM_MXU:
                    edges = jnp.concatenate([elat[k, rows, :] for k in range(6)], axis=1)
                    total = dot(edges, jnp.concatenate([perms[2]] * 6, axis=0))
                else:
                    total = elat[0, rows, :].astype(F32)
                    for k in range(1, 6):
                        total = total + elat[k, rows, :].astype(F32)
                pre = dot(node, wni[layer, 0:256, :]) + dot(total.astype(BF16), wni[layer, 256:512, :])
                new = residual(node, norm(dot(silu_of_half(pre), wno[layer])))
                hcur[sub:sub + SUB // 64] = new.reshape(SUB // 64, 64, 256)

            @pl.when(layer < layers - 2)
            def _():
                send_halo(1 - slot)
            return carry

        def forecast(step, carry):
            def encode(it, carry):
                esums = []
                nodes = []
                dests = [lax.rem(me + PER * it + 1 + q, group) for q in range(PER)]
                for dest in dests:
                    for half in range(2):
                        chunk = half * group + dest
                        rows = pl.ds(pl.multiple_of(chunk * 256, 256), 256)
                        mrows = pl.ds(pl.multiple_of(chunk * 64, 64), 64)
                        feats = jnp.concatenate([xs[step, rows, :], xs[step + 1, rows, :]], axis=1)
                        pre = dot(feats, wg[step, 0:256, :]) + dot(fm[rows, :], wg[step, 256:384, :])
                        lat = norm(dot(silu_of_half(pre), wembo[0])).astype(BF16)
                        glat[rows, :] = lat
                        node = mlat[mrows, :]
                        term = dot(node, wei[0, 512:768, :])
                        old = g2m[rows, :]
                        pre = dot(old, wei[0, 0:256, :]) + dot(lat, wei[0, 256:512, :])
                        pre = pre + jnp.concatenate([term] * 4, axis=0)
                        edge = residual(old, norm(dot(silu_of_half(pre), weo[0]))).astype(F32)
                        esums.append((edge[0:64] + edge[64:128] + edge[128:192] + edge[192:256]).astype(BF16))
                        nodes.append(node)
                for lo in range(0, 2 * PER, 4):
                    node = jnp.concatenate(nodes[lo:lo + 4], axis=0)
                    pre = dot(node, wni[0, 0:256, :]) + dot(jnp.concatenate(esums[lo:lo + 4], axis=0), wni[0, 256:512, :])
                    new = residual(node, norm(dot(silu_of_half(pre), wno[0])))
                    for q in range(4):
                        hsend[q % 2, dests[(lo + q) // 2]] = new[q * 64:q * 64 + 64]
                for q in range(PER - 1):
                    for half in range(2):
                        en_copy(PER * it + 1 + q, half).start()

                @pl.when(it < group // PER - 1)
                def _():
                    for half in range(2):
                        en_copy(PER * it + PER, half).start()
                return carry

            lax.fori_loop(0, group // PER, encode, 0)

            @pl.when(step == 0)
            def _():
                for half in range(2):
                    for hop in range(1, group):
                        ef_arrival(lax.rem(me + hop, group), half).wait_recv()
                    ef_keep(half).wait()

                def embed_edges(k, carry):
                    for sub in range(0, blocks, 4):
                        feats = efl[sub:sub + 4].reshape(256, 128)
                        ebase[k, sub * 64:sub * 64 + 256, :] = norm(dot(silu_of_half(dot(feats, wemb[3 + k])), wembo[4])).astype(BF16)
                    return carry

                lax.fori_loop(0, 6, embed_edges, 0)
                for hop in range(1, group):
                    for half in range(2):
                        ef_copy(hop, half).wait_send()

            elat[...] = ebase[...]
            for hop in range(1, group):
                for half in range(2):
                    en_arrival(lax.rem(me + hop, group), half).wait_recv()
            for hop in range(1, group):
                for half in range(2):
                    en_copy(hop, half).wait_send()
            hcur[...] = hin[...]
            for half in range(2):
                hcur[block_of(me, 1 + half)] = hsend[half, me]
            send_halo(1)
            lax.fori_loop(1, layers - 1, mesh_layer, 0)
            for hop in range(1, group):
                for half in range(2):
                    de_copy(hop, half).start()
            for half in range(2):
                hd[half, me] = hcur[block_of(me, 1 + half)]

            def self_update(it, carry):
                for sub in range(4):
                    rows = pl.ds(pl.multiple_of((it * 4 + sub) * 256, 256), 256)
                    old = glat[rows, :]
                    gcur[rows, :] = residual(old, norm(dot(silu_of_half(dot(old, wsh[0])), wgs[1])))
                return carry

            lax.fori_loop(0, 4, self_update, 0)

            @pl.when(step == 0)
            def _():
                x_copy.wait()

            def decode(it, carry):
                last = layers - 1
                for q in range(PER - 1):
                    for half in range(2):
                        de_arrival(lax.rem(me + PER * it + 1 + q, group), half).wait_recv()

                @pl.when(it < group // PER - 1)
                def _():
                    for half in range(2):
                        de_arrival(lax.rem(me + PER * it + PER, group), half).wait_recv()

                work = []
                for q in range(PER):
                    source = lax.rem(me + PER * it + 1 + q, group)
                    for half in range(2):
                        rows = pl.ds(pl.multiple_of((half * group + source) * 256, 256), 256)
                        work.append((rows, hd[half, source], m2g[rows, :], gcur[rows, :], xst[step, rows, :]))
                done = []
                for rows, node, old, grid, state in work:
                    term = dot(node, wei[last, 256:512, :])
                    pre = dot(old, wei[last, 0:256, :]) + dot(grid, wei[last, 512:768, :])
                    pre = pre + jnp.concatenate([term] * 4, axis=0)
                    edge = residual(old, norm(dot(silu_of_half(pre), weo[last])))
                    pre = dot(grid, wni[last, 0:256, :]) + dot(edge, wni[last, 256:512, :])
                    out = residual(grid, norm(dot(silu_of_half(pre), wno[last])))
                    hidden = silu_of_half(dot(out, wsh[1]))
                    hidden = dot(perms[1], hidden).astype(BF16)
                    new = state + stats[3:4, :] * dot(hidden, wof[...]) + stats[2:3, :]
                    scaled = ((new - stats[0:1, :]) / stats[1:2, :]).astype(BF16)
                    done.append((rows, new, dot(perms[0], scaled).astype(BF16)))
                for rows, new, scaled in done:
                    xst[step + 1, rows, :] = new
                    xs[2, rows, 0:scaled.shape[1]] = scaled
                return carry

            lax.fori_loop(0, group // PER, decode, 0)
            for hop in range(1, group):
                for half in range(2):
                    de_copy(hop, half).wait_send()

            @pl.when(step == 0)
            def _():
                pltpu.make_async_copy(xst.at[1], out0, osem.at[0]).start()
            return carry

        lax.fori_loop(0, 2, forecast, 0)
        final = pltpu.make_async_copy(xst.at[2], out1, osem.at[1])
        final.start()
        pltpu.make_async_copy(xst.at[1], out0, osem.at[0]).wait()
        final.wait()

    def shift_pairs(hop_count):
        return [(source, (source + hop_count) % group) for source in range(group)]

    def local_run(x_prev, x_cur, forcing, grid_static, g2m_feat, m2g_feat, mesh_feat, mesh_edge_feat, norm_stats, w_grid_in, w_mesh_in, w_eemb_in, w_embed_out, w_edge_in, w_edge_out, w_node_in, w_node_out, w_grid_self, w_out_hidden, w_out_final):
        grid_dev, variables = x_prev.shape
        mesh_dev = mesh_feat.shape[0]
        latent = w_embed_out.shape[-1]
        blocks = 2 * group
        half_grid = grid_dev // 2
        half_mesh = mesh_dev // 2

        def shifted(values, half):
            head = lax.ppermute(values[:half], "gp", shift_pairs(-1))
            return jnp.concatenate([values[half:], head], axis=0)

        def in_order(values):
            lanes = values.shape[-1]
            values = values.reshape(2, group, 8, 8, lanes).transpose(0, 1, 3, 2, 4)
            return values.reshape(2, group, 64, lanes)

        def lane_pad(values, width):
            return jnp.pad(values, [(0, 0)] * (values.ndim - 1) + [(0, width - values.shape[-1])])

        g2m_here = shifted(g2m_feat, half_grid)
        mesh_here = shifted(mesh_feat, half_mesh)
        misc = jnp.concatenate([forcing[:, 0, :], forcing[:, 1, :], grid_static, g2m_here, m2g_feat], axis=1)
        force = forcing.shape[-1]
        static = grid_static.shape[-1]
        edge_lanes = g2m_feat.shape[-1]
        scale = lambda x: (x - norm_stats[0]) / norm_stats[1]
        feats = jnp.concatenate([lane_pad(scale(x_prev), 128), lane_pad(scale(x_cur), 128), lane_pad(misc, 128)], axis=1).astype(BF16)
        mesh_rows = lane_pad(in_order(mesh_here).astype(BF16), 128).reshape(mesh_dev, 128)
        edge_rows = lane_pad(in_order(mesh_edge_feat.reshape(mesh_dev, -1)).astype(BF16), 128)

        def placed(rows, start, height):
            return jnp.pad(rows, ((start, height - start - rows.shape[0]), (0, 0)))

        w_force = w_grid_in[2 * variables:2 * variables + force]
        w_static = w_grid_in[2 * variables + force:]
        w_state = placed(w_grid_in[:variables], 0, 384) + placed(w_grid_in[variables:2 * variables], 128, 384) + placed(w_static, 256 + 2 * force, 384)
        w_grid = 0.5 * jnp.stack([w_state + placed(w_force, 256 + force * s, 384) for s in range(2)])
        at_g2m = 2 * force + static
        w_embed = 0.5 * jnp.stack([placed(w_eemb_in[0], at_g2m, 128), placed(w_eemb_in[1], at_g2m + edge_lanes, 128), placed(w_mesh_in, 0, 128)]
                            + [placed(w_eemb_in[2], edge_lanes * k, 128) for k in range(6)])
        perms = jnp.asarray(row_permutation(), BF16)

        vmem = pl.BlockSpec(memory_space=pltpu.VMEM)
        anywhere = pl.BlockSpec(memory_space=pl.ANY)
        state = jax.ShapeDtypeStruct((grid_dev, variables), F32)
        dma = pltpu.SemaphoreType.DMA
        return pl.pallas_call(
            kernel,
            out_shape=(state, state),
            in_specs=[vmem, anywhere, anywhere] + [vmem] * 6 + [anywhere] * 4 + [vmem] * 3,
            out_specs=(anywhere, anywhere),
            scratch_shapes=[
                pltpu.VMEM(w_edge_in.shape, BF16), pltpu.VMEM(w_edge_out.shape, BF16),
                pltpu.VMEM(w_node_in.shape, BF16), pltpu.VMEM(w_node_out.shape, BF16),
                pltpu.VMEM((3, grid_dev, variables), F32), pltpu.VMEM((3, grid_dev, 128), BF16), pltpu.VMEM((grid_dev, 128), BF16),
                pltpu.VMEM((grid_dev, latent), BF16), pltpu.VMEM((grid_dev, latent), BF16), pltpu.VMEM((grid_dev, latent), BF16),
                pltpu.VMEM((grid_dev, latent), BF16),
                pltpu.VMEM((mesh_dev, latent), BF16), pltpu.VMEM((blocks, 64, 128), BF16),
                pltpu.VMEM((6, mesh_dev, latent), BF16), pltpu.VMEM((6, mesh_dev, latent), BF16),
                pltpu.VMEM((2, group, 64, latent), BF16), pltpu.VMEM((blocks, 64, latent), BF16),
                pltpu.VMEM((blocks, 64, latent), BF16), pltpu.VMEM((2, group, 64, latent), BF16),
                pltpu.VMEM((blocks, 80, latent), F32), pltpu.VMEM((mesh_dev, latent), F32),
                pltpu.VMEM((2, 2, blocks, latent), BF16), pltpu.VMEM((2, 2, blocks, latent), BF16), pltpu.VMEM((2, blocks, latent), F32), pltpu.VMEM((2, latent, latent), BF16),
                dma((4,)), dma, dma((2,)), dma((group, 2)), dma((group, 2)), dma((group, 2)), dma((group, 2)),
                dma((group, 2)), dma((group, 2)), dma((2, 2)), dma((2, 2)),
            ],
            compiler_params=pltpu.CompilerParams(collective_id=0, has_side_effects=True, flags=FLAGS, vmem_limit_bytes=67043328),
        )(feats, x_cur, edge_rows, mesh_rows, norm_stats, perms, w_grid, w_embed, w_embed_out, w_edge_in, w_edge_out, w_node_in, w_node_out,
          w_grid_self, w_out_hidden, w_out_final)

    row_spec = P(("dp", "gp"))
    edge_spec = P(("dp", "gp"), None, None)
    whole = P()
    in_specs = (row_spec, row_spec, edge_spec, row_spec, row_spec, row_spec, row_spec, edge_spec, whole) + (whole,) * 11
    return jax.shard_map(local_run, mesh=mesh, in_specs=in_specs, out_specs=(row_spec, row_spec), check_vma=False)
```

```python
import jax
import jax.numpy as jnp
import numpy as np
from jax import lax
from jax.experimental import pallas as pl
from jax.experimental.pallas import tpu as pltpu
from jax.sharding import PartitionSpec as P

MESH_ID = pl.DeviceIdType.MESH
F32 = jnp.float32
BF16 = jnp.bfloat16
SUB = 256
TAIL = 256
PER = 4
WIDTH = 3
TAIL_WIDTH = 4
FLAGS = {}


def dot(a, b):
    return jnp.dot(a, b, preferred_element_type=F32)


def silu_of_half(half):
    return (half * jnp.tanh(half) + half).astype(BF16)


def norm(y):
    z = y - jnp.mean(y, axis=-1, keepdims=True)
    return z * lax.rsqrt(jnp.mean(z * z, axis=-1, keepdims=True) + 1e-5)


def staggered(tasks, width):
    waiting = list(tasks)
    active = []
    while waiting or active:
        if waiting and len(active) < width:
            active.append(waiting.pop(0))
        for task in list(active):
            if next(task, "done") == "done":
                active.remove(task)


def together(tasks):
    active = list(tasks)
    while active:
        active = [task for task in active if next(task, "done") != "done"]


def residual(base, update):
    return (base.astype(F32) + update).astype(BF16)


def row_permutation():
    perm = np.zeros((256, 256), np.float32)
    for r in range(4):
        for j in range(8):
            for i in range(8):
                perm[r * 64 + j * 8 + i, (i * 8 + j) * 4 + r] = 1.0
    return np.stack([perm, perm.T])


def solution(mesh):
    group = mesh.shape["gp"]

    def kernel(f0, xc_hbm, ef_hbm, mf, stats, perms, wg, wemb, wembo, wei_hbm, weo_hbm, wni_hbm, wno_hbm, wgs, woh, wof,
               out0, out1,
               wei, weo, wni, wno, xst, xs, fm, g2m, m2g, glat, gcur, mlat, efl, ebase, elat, hsend, hin, hcur, hd,
               proj, recv, halo_s, halo_r, stage, wsh,
               wsem, xsem, osem, ef_s, ef_r, en_s, en_r, de_s, de_r, ha_s, ha_r):
        me = lax.axis_index("gp")
        left = lax.rem(me + group - 1, group)
        right = lax.rem(me + 1, group)
        blocks = 2 * group
        layers = wei_hbm.shape[0]

        barrier = pltpu.get_barrier_semaphore()
        for hop in range(1, group):
            pl.semaphore_signal(barrier, inc=1, device_id={"gp": lax.rem(me + hop, group)}, device_id_type=MESH_ID)

        weight_copies = [pltpu.make_async_copy(src, dst, wsem.at[i]) for i, (src, dst) in enumerate(
            [(wei_hbm, wei), (weo_hbm, weo), (wni_hbm, wni), (wno_hbm, wno)])]
        x_copy = pltpu.make_async_copy(xc_hbm, xst.at[0], xsem)
        x_copy.start()
        for copy in weight_copies:
            copy.start()
        pl.semaphore_wait(barrier, group - 1)

        def block_of(device, half):
            return lax.rem(2 * device + half, blocks)

        def ef_copy(hop, half):
            dest = lax.rem(me + hop, group)
            return pltpu.make_async_remote_copy(
                src_ref=ef_hbm.at[half, dest], dst_ref=efl.at[2 * me + half], send_sem=ef_s.at[dest, half],
                recv_sem=ef_r.at[me, half], device_id={"gp": dest}, device_id_type=MESH_ID)

        def ef_keep(half):
            return pltpu.make_async_copy(ef_hbm.at[half, me], efl.at[2 * me + half], ef_r.at[me, half])

        for half in range(2):
            for hop in range(1, group):
                ef_copy(hop, half).start()
            ef_keep(half).start()

        def embed_task(rows):
            feats = dot(perms[0], f0[rows, :])
            yield
            feats = feats.astype(BF16)
            xs[0, rows, :] = feats[:, 0:128]
            xs[1, rows, :] = feats[:, 128:256]
            misc = feats[:, 256:384]
            fm[rows, :] = misc
            first = dot(misc, wemb[0])
            second = dot(misc, wemb[1])
            yield
            first = dot(silu_of_half(first), wembo[2])
            second = dot(silu_of_half(second), wembo[3])
            yield
            g2m[rows, :] = norm(first).astype(BF16)
            m2g[rows, :] = norm(second).astype(BF16)

        def embed_rows(it, carry):
            together(embed_task(pl.ds(pl.multiple_of((it * 4 + sub) * 256, 256), 256)) for sub in range(4))
            return carry

        lax.fori_loop(0, 4, embed_rows, 0)

        def plain_task(get, put, w_first, w_second):
            y = dot(get(), w_first)
            yield
            y = dot(silu_of_half(y), w_second)
            yield
            put(norm(y))

        def mesh_task(rows):
            def put(y):
                mlat[rows, :] = y.astype(BF16)
            return plain_task(lambda: mf[rows, :], put, wemb[2], wembo[1])

        together(mesh_task(pl.ds(sub * 256, 256)) for sub in range(4))
        xs[2] = jnp.zeros(xs.shape[1:], BF16)
        for copy in weight_copies:
            copy.wait()

        def halve(layer, carry):
            wei[layer] = wei[layer] * 0.5
            wni[layer] = wni[layer] * 0.5
            return carry

        lax.fori_loop(0, layers, halve, 0)
        wsh[0] = wgs[0] * 0.5
        wsh[1] = woh[...] * 0.5

        def en_copy(hop, half):
            dest = lax.rem(me + hop, group)
            return pltpu.make_async_remote_copy(
                src_ref=hsend.at[half, dest], dst_ref=hin.at[block_of(me, 1 + half)], send_sem=en_s.at[dest, half],
                recv_sem=en_r.at[me, half], device_id={"gp": dest}, device_id_type=MESH_ID)

        def de_copy(hop, half):
            dest = lax.rem(me + hop, group)
            return pltpu.make_async_remote_copy(
                src_ref=hcur.at[block_of(dest, 1 + half)], dst_ref=hd.at[half, me], send_sem=de_s.at[dest, half],
                recv_sem=de_r.at[me, half], device_id={"gp": dest}, device_id_type=MESH_ID)

        def en_arrival(source, half):
            return pltpu.make_async_remote_copy(
                src_ref=hsend.at[half, me], dst_ref=hin.at[block_of(source, 1 + half)], send_sem=en_s.at[me, half],
                recv_sem=en_r.at[source, half], device_id={"gp": left}, device_id_type=MESH_ID)

        def de_arrival(source, half):
            return pltpu.make_async_remote_copy(
                src_ref=hcur.at[0], dst_ref=hd.at[half, source], send_sem=de_s.at[me, half],
                recv_sem=de_r.at[source, half], device_id={"gp": left}, device_id_type=MESH_ID)

        def ef_arrival(source, half):
            return pltpu.make_async_remote_copy(
                src_ref=ef_hbm.at[half, me], dst_ref=efl.at[2 * source + half], send_sem=ef_s.at[me, half],
                recv_sem=ef_r.at[source, half], device_id={"gp": left}, device_id_type=MESH_ID)

        def halo_copies(slot):
            return [pltpu.make_async_remote_copy(
                src_ref=halo_s.at[slot, side], dst_ref=halo_r.at[slot, 1 - side], send_sem=ha_s.at[slot, side],
                recv_sem=ha_r.at[slot, 1 - side], device_id={"gp": (left, right)[side]}, device_id_type=MESH_ID)
                for side in range(2)]

        def send_halo(slot):
            for b in range(blocks):
                stage[0, b:b + 1, :] = hcur[b, 0:16, :].astype(F32)[0:1]
                stage[1, b:b + 1, :] = hcur[b, 48:64, :].astype(F32)[15:16]
            halo_s[slot, 0] = stage[0].astype(BF16)
            halo_s[slot, 1] = stage[1].astype(BF16)
            for copy in halo_copies(slot):
                copy.start()

        def edge_task(layer, k, sub, size, send):
            rows = slice(sub, sub + size)
            old = elat[k, rows, :]
            pre = dot(old, wei[layer, 0:256, :]) + (send + recv[rows, :])
            yield
            y = dot(silu_of_half(pre), weo[layer])
            yield
            elat[k, rows, :] = residual(old, norm(y))

        def project(layer, lo, hi):
            h = hcur[lo:hi].reshape((hi - lo) * 64, 256)
            return dot(h, wei[layer, 256:512, :]), dot(h, wei[layer, 512:768, :])

        def put_projections(lo, hi, send, receive):
            proj[lo:hi, 8:72, :] = send.reshape(hi - lo, 64, 256)
            recv[lo * 64:hi * 64, :] = receive

        def tail_task(layer, lo, hi):
            size = (hi - lo) * 64
            rows = slice(lo * 64, hi * 64)
            olds = [elat[k, rows, :] for k in range(2)]
            sends = [proj[lo:hi, 16:80, :].reshape(size, 256), proj[lo:hi, 0:64, :].reshape(size, 256)]
            pres = [dot(old, wei[layer, 0:256, :]) + (send + recv[rows, :]) for old, send in zip(olds, sends)]
            total = elat[2, rows, :].astype(F32)
            for k in range(3, 6):
                total = total + elat[k, rows, :].astype(F32)
            yield
            ys = [dot(silu_of_half(pre), weo[layer]) for pre in pres]
            yield
            for k in range(2):
                new = residual(olds[k], norm(ys[k]))
                elat[k, rows, :] = new
                total = total + new.astype(F32)
            node = hcur[lo:hi].reshape(size, 256)
            pre = dot(node, wni[layer, 0:256, :]) + dot(total.astype(BF16), wni[layer, 256:512, :])
            yield
            y = dot(silu_of_half(pre), wno[layer])
            yield
            new = residual(node, norm(y))
            hcur[lo:hi] = new.reshape(hi - lo, 64, 256)
            send = dot(new, wei[layer + 1, 256:512, :])
            receive = dot(new, wei[layer + 1, 512:768, :])
            yield
            put_projections(lo, hi, send, receive)

        def rolled(shift, sub, size):
            lo, count = sub // 64, size // 64
            picks = [(lo + q + shift) % blocks for q in range(count)]
            return jnp.concatenate([proj[b, 8:72, :] for b in picks], axis=0)

        def mesh_layer(layer, carry):
            slot = lax.rem(layer, 2)
            staggered((edge_task(layer, k, sub, SUB, rolled(shift, sub, SUB))
                       for k, shift in ((2, 1), (3, -1), (4, 4), (5, -4)) for sub in range(0, blocks * 64, SUB)), WIDTH)
            for copy in halo_copies(slot):
                copy.wait_recv()
            for copy in halo_copies(slot):
                copy.wait_send()
            edge_proj = dot(halo_r[slot].reshape(32, 256), wei[layer, 256:512, :])
            low = edge_proj[0:16]
            high = edge_proj[16:32]
            stage[0] = jnp.where(me == 0, jnp.concatenate([low[15:16], low[0:15]], axis=0), low)
            stage[1] = jnp.where(me == group - 1, jnp.concatenate([high[1:16], high[0:1]], axis=0), high)
            sublane = lax.broadcasted_iota(jnp.int32, (8, 256), 0)
            for b in range(blocks):
                proj[b, 0:8, :] = jnp.where(sublane == 0, stage[0, b:b + 1, :], pltpu.roll(proj[b, 64:72, :], 1, 0))
                proj[b, 72:80, :] = jnp.where(sublane == 7, stage[1, b:b + 1, :], pltpu.roll(proj[b, 8:16, :], 7, 0))
            staggered((tail_task(layer, lo, lo + TAIL // 64) for lo in range(0, blocks, TAIL // 64)), TAIL_WIDTH)

            @pl.when(layer < layers - 2)
            def _():
                send_halo(1 - slot)
            return carry

        def forecast(step, carry):
            def encode_task(dest, half):
                chunk = half * group + dest
                rows = pl.ds(pl.multiple_of(chunk * 256, 256), 256)
                feats = jnp.concatenate([xs[step, rows, :], xs[step + 1, rows, :]], axis=1)
                node = mlat[pl.ds(pl.multiple_of(chunk * 64, 64), 64), :]
                old = g2m[rows, :]
                pre = dot(feats, wg[step, 0:256, :]) + dot(fm[rows, :], wg[step, 256:384, :])
                yield
                y = dot(silu_of_half(pre), wembo[0])
                yield
                lat = norm(y).astype(BF16)
                glat[rows, :] = lat
                pre = dot(old, wei[0, 0:256, :]) + dot(lat, wei[0, 256:512, :])
                term = dot(node, wei[0, 512:768, :])
                yield
                pre = pre + jnp.concatenate([term] * 4, axis=0)
                y = dot(silu_of_half(pre), weo[0])
                yield
                edge = residual(old, norm(y)).astype(F32)
                return node, (edge[0:64] + edge[64:128] + edge[128:192] + edge[192:256]).astype(BF16)

            def encode_group(pairs):
                results = []

                def run(dest, half):
                    results.append((yield from encode_task(dest, half)))

                active = [run(dest, half) for dest, half in pairs]
                while active:
                    active = [task for task in active if next(task, "done") != "done"]
                    yield
                node = jnp.concatenate([r[0] for r in results], axis=0)
                esum = jnp.concatenate([r[1] for r in results], axis=0)
                pre = dot(node, wni[0, 0:256, :]) + dot(esum, wni[0, 256:512, :])
                yield
                y = dot(silu_of_half(pre), wno[0])
                yield
                new = residual(node, norm(y))
                for q, (dest, half) in enumerate(pairs):
                    hsend[half, dest] = new[q * 64:q * 64 + 64]

            def encode(it, carry):
                dests = [lax.rem(me + PER * it + 1 + q, group) for q in range(PER)]
                pairs = [(dest, half) for dest in dests for half in range(2)]
                staggered((encode_group(pairs[lo:lo + 4]) for lo in range(0, 2 * PER, 4)), 4)
                for q in range(PER - 1):
                    for half in range(2):
                        en_copy(PER * it + 1 + q, half).start()

                @pl.when(it < group // PER - 1)
                def _():
                    for half in range(2):
                        en_copy(PER * it + PER, half).start()
                return carry

            lax.fori_loop(0, group // PER, encode, 0)

            @pl.when(step == 0)
            def _():
                for half in range(2):
                    for hop in range(1, group):
                        ef_arrival(lax.rem(me + hop, group), half).wait_recv()
                    ef_keep(half).wait()

                def embed_edges(k, carry):
                    def edge_embed_task(sub):
                        def put(y):
                            ebase[k, sub * 64:sub * 64 + 256, :] = y.astype(BF16)
                        return plain_task(lambda: efl[sub:sub + 4].reshape(256, 128), put, wemb[3 + k], wembo[4])

                    together(edge_embed_task(sub) for sub in range(0, blocks, 4))
                    return carry

                lax.fori_loop(0, 6, embed_edges, 0)
                for hop in range(1, group):
                    for half in range(2):
                        ef_copy(hop, half).wait_send()

            elat[...] = ebase[...]
            for hop in range(1, group):
                for half in range(2):
                    en_arrival(lax.rem(me + hop, group), half).wait_recv()
            for hop in range(1, group):
                for half in range(2):
                    en_copy(hop, half).wait_send()
            hcur[...] = hin[...]
            for half in range(2):
                hcur[block_of(me, 1 + half)] = hsend[half, me]
            send_halo(1)
            put_projections(0, blocks, *project(1, 0, blocks))
            lax.fori_loop(1, layers - 1, mesh_layer, 0)
            for hop in range(1, group):
                for half in range(2):
                    de_copy(hop, half).start()
            for half in range(2):
                hd[half, me] = hcur[block_of(me, 1 + half)]

            def self_task(rows):
                old = glat[rows, :]

                def put(y):
                    gcur[rows, :] = residual(old, y)
                return plain_task(lambda: old, put, wsh[0], wgs[1])

            def self_update(it, carry):
                together(self_task(pl.ds(pl.multiple_of((it * 4 + sub) * 256, 256), 256)) for sub in range(4))
                return carry

            lax.fori_loop(0, 4, self_update, 0)

            @pl.when(step == 0)
            def _():
                x_copy.wait()

            def decode(it, carry):
                last = layers - 1
                for q in range(PER - 1):
                    for half in range(2):
                        de_arrival(lax.rem(me + PER * it + 1 + q, group), half).wait_recv()

                @pl.when(it < group // PER - 1)
                def _():
                    for half in range(2):
                        de_arrival(lax.rem(me + PER * it + PER, group), half).wait_recv()

                work = []
                for q in range(PER):
                    source = lax.rem(me + PER * it + 1 + q, group)
                    for half in range(2):
                        rows = pl.ds(pl.multiple_of((half * group + source) * 256, 256), 256)
                        work.append((rows, hd[half, source], m2g[rows, :], gcur[rows, :], xst[step, rows, :]))
                def decode_task(rows, node, old, grid, state):
                    pre = dot(old, wei[last, 0:256, :]) + dot(grid, wei[last, 512:768, :])
                    term = dot(node, wei[last, 256:512, :])
                    yield
                    pre = pre + jnp.concatenate([term] * 4, axis=0)
                    y = dot(silu_of_half(pre), weo[last])
                    yield
                    edge = residual(old, norm(y))
                    pre = dot(grid, wni[last, 0:256, :]) + dot(edge, wni[last, 256:512, :])
                    yield
                    y = dot(silu_of_half(pre), wno[last])
                    yield
                    out = residual(grid, norm(y))
                    pre = dot(out, wsh[1])
                    yield
                    hidden = dot(perms[1], silu_of_half(pre))
                    yield
                    p = dot(hidden.astype(BF16), wof[...])
                    yield
                    new = state + stats[3:4, :] * p + stats[2:3, :]
                    scaled = dot(perms[0], ((new - stats[0:1, :]) / stats[1:2, :]).astype(BF16))
                    yield
                    xst[step + 1, rows, :] = new
                    xs[2, rows, 0:new.shape[1]] = scaled.astype(BF16)

                staggered((decode_task(*args) for args in work), 2 * PER)
                return carry

            lax.fori_loop(0, group // PER, decode, 0)
            for hop in range(1, group):
                for half in range(2):
                    de_copy(hop, half).wait_send()

            @pl.when(step == 0)
            def _():
                pltpu.make_async_copy(xst.at[1], out0, osem.at[0]).start()
            return carry

        lax.fori_loop(0, 2, forecast, 0)
        final = pltpu.make_async_copy(xst.at[2], out1, osem.at[1])
        final.start()
        pltpu.make_async_copy(xst.at[1], out0, osem.at[0]).wait()
        final.wait()

    def shift_pairs(hop_count):
        return [(source, (source + hop_count) % group) for source in range(group)]

    def local_run(x_prev, x_cur, forcing, grid_static, g2m_feat, m2g_feat, mesh_feat, mesh_edge_feat, norm_stats, w_grid_in, w_mesh_in, w_eemb_in, w_embed_out, w_edge_in, w_edge_out, w_node_in, w_node_out, w_grid_self, w_out_hidden, w_out_final):
        grid_dev, variables = x_prev.shape
        mesh_dev = mesh_feat.shape[0]
        latent = w_embed_out.shape[-1]
        blocks = 2 * group
        half_grid = grid_dev // 2
        half_mesh = mesh_dev // 2

        def shifted(values, half):
            head = lax.ppermute(values[:half], "gp", shift_pairs(-1))
            return jnp.concatenate([values[half:], head], axis=0)

        def in_order(values):
            lanes = values.shape[-1]
            values = values.reshape(2, group, 8, 8, lanes).transpose(0, 1, 3, 2, 4)
            return values.reshape(2, group, 64, lanes)

        def lane_pad(values, width):
            return jnp.pad(values, [(0, 0)] * (values.ndim - 1) + [(0, width - values.shape[-1])])

        g2m_here = shifted(g2m_feat, half_grid)
        mesh_here = shifted(mesh_feat, half_mesh)
        misc = jnp.concatenate([forcing[:, 0, :], forcing[:, 1, :], grid_static, g2m_here, m2g_feat], axis=1)
        force = forcing.shape[-1]
        static = grid_static.shape[-1]
        edge_lanes = g2m_feat.shape[-1]
        scale = lambda x: (x - norm_stats[0]) / norm_stats[1]
        feats = jnp.concatenate([lane_pad(scale(x_prev), 128), lane_pad(scale(x_cur), 128), lane_pad(misc, 128)], axis=1).astype(BF16)
        mesh_rows = lane_pad(in_order(mesh_here).astype(BF16), 128).reshape(mesh_dev, 128)
        edge_rows = lane_pad(in_order(mesh_edge_feat.reshape(mesh_dev, -1)).astype(BF16), 128)

        def placed(rows, start, height):
            return jnp.pad(rows, ((start, height - start - rows.shape[0]), (0, 0)))

        w_force = w_grid_in[2 * variables:2 * variables + force]
        w_static = w_grid_in[2 * variables + force:]
        w_state = placed(w_grid_in[:variables], 0, 384) + placed(w_grid_in[variables:2 * variables], 128, 384) + placed(w_static, 256 + 2 * force, 384)
        w_grid = 0.5 * jnp.stack([w_state + placed(w_force, 256 + force * s, 384) for s in range(2)])
        at_g2m = 2 * force + static
        w_embed = 0.5 * jnp.stack([placed(w_eemb_in[0], at_g2m, 128), placed(w_eemb_in[1], at_g2m + edge_lanes, 128), placed(w_mesh_in, 0, 128)]
                            + [placed(w_eemb_in[2], edge_lanes * k, 128) for k in range(6)])
        perms = jnp.asarray(row_permutation(), BF16)

        vmem = pl.BlockSpec(memory_space=pltpu.VMEM)
        anywhere = pl.BlockSpec(memory_space=pl.ANY)
        state = jax.ShapeDtypeStruct((grid_dev, variables), F32)
        dma = pltpu.SemaphoreType.DMA
        return pl.pallas_call(
            kernel,
            out_shape=(state, state),
            in_specs=[vmem, anywhere, anywhere] + [vmem] * 6 + [anywhere] * 4 + [vmem] * 3,
            out_specs=(anywhere, anywhere),
            scratch_shapes=[
                pltpu.VMEM(w_edge_in.shape, BF16), pltpu.VMEM(w_edge_out.shape, BF16),
                pltpu.VMEM(w_node_in.shape, BF16), pltpu.VMEM(w_node_out.shape, BF16),
                pltpu.VMEM((3, grid_dev, variables), F32), pltpu.VMEM((3, grid_dev, 128), BF16), pltpu.VMEM((grid_dev, 128), BF16),
                pltpu.VMEM((grid_dev, latent), BF16), pltpu.VMEM((grid_dev, latent), BF16), pltpu.VMEM((grid_dev, latent), BF16),
                pltpu.VMEM((grid_dev, latent), BF16),
                pltpu.VMEM((mesh_dev, latent), BF16), pltpu.VMEM((blocks, 64, 128), BF16),
                pltpu.VMEM((6, mesh_dev, latent), BF16), pltpu.VMEM((6, mesh_dev, latent), BF16),
                pltpu.VMEM((2, group, 64, latent), BF16), pltpu.VMEM((blocks, 64, latent), BF16),
                pltpu.VMEM((blocks, 64, latent), BF16), pltpu.VMEM((2, group, 64, latent), BF16),
                pltpu.VMEM((blocks, 80, latent), F32), pltpu.VMEM((mesh_dev, latent), F32),
                pltpu.VMEM((2, 2, blocks, latent), BF16), pltpu.VMEM((2, 2, blocks, latent), BF16), pltpu.VMEM((2, blocks, latent), F32), pltpu.VMEM((2, latent, latent), BF16),
                dma((4,)), dma, dma((2,)), dma((group, 2)), dma((group, 2)), dma((group, 2)), dma((group, 2)),
                dma((group, 2)), dma((group, 2)), dma((2, 2)), dma((2, 2)),
            ],
            compiler_params=pltpu.CompilerParams(collective_id=0, has_side_effects=True, flags=FLAGS, vmem_limit_bytes=67043328),
        )(feats, x_cur, edge_rows, mesh_rows, norm_stats, perms, w_grid, w_embed, w_embed_out, w_edge_in, w_edge_out, w_node_in, w_node_out,
          w_grid_self, w_out_hidden, w_out_final)

    row_spec = P(("dp", "gp"))
    edge_spec = P(("dp", "gp"), None, None)
    whole = P()
    in_specs = (row_spec, row_spec, edge_spec, row_spec, row_spec, row_spec, row_spec, edge_spec, whole) + (whole,) * 11
    return jax.shard_map(local_run, mesh=mesh, in_specs=in_specs, out_specs=(row_spec, row_spec), check_vma=False)
```

```python
import jax
import jax.numpy as jnp
import numpy as np
from jax import lax
from jax.experimental import pallas as pl
from jax.experimental.pallas import tpu as pltpu
from jax.sharding import PartitionSpec as P

MESH_ID = pl.DeviceIdType.MESH
F32 = jnp.float32
BF16 = jnp.bfloat16
SUB = 256
TAIL = 256
PER = 4
WIDTH = 3
TAIL_WIDTH = 4
FLAGS = {}


def dot(a, b):
    return jnp.dot(a, b, preferred_element_type=F32)


def dot_t(a, b):
    return lax.dot_general(a, b, (((1,), (1,)), ((), ())), preferred_element_type=F32)


def silu_of_half(half):
    return (half * jnp.tanh(half) + half).astype(BF16)


def norm(y):
    z = y - jnp.mean(y, axis=-1, keepdims=True)
    return z * lax.rsqrt(jnp.mean(z * z, axis=-1, keepdims=True) + 1e-5)


def staggered(tasks, width):
    waiting = list(tasks)
    active = []
    while waiting or active:
        if waiting and len(active) < width:
            active.append(waiting.pop(0))
        for task in list(active):
            if next(task, "done") == "done":
                active.remove(task)


def together(tasks):
    active = list(tasks)
    while active:
        active = [task for task in active if next(task, "done") != "done"]


def residual(base, update):
    return (base.astype(F32) + update).astype(BF16)


def row_permutation():
    perm = np.zeros((256, 256), np.float32)
    for r in range(4):
        for j in range(8):
            for i in range(8):
                perm[r * 64 + j * 8 + i, (i * 8 + j) * 4 + r] = 1.0
    swap = np.zeros((256, 256), np.float32)
    for g in range(4):
        for j in range(8):
            for i in range(8):
                swap[g * 64 + j * 8 + i, g * 64 + i * 8 + j] = 1.0
    return np.stack([perm, perm.T, swap])


def solution(mesh):
    group = mesh.shape["gp"]

    def kernel(xp_hbm, xc_hbm, force_t, static_t, g2m_t, m2g_t, mesh_t, edge_t, stats, perms, w_grid, w_mesh, w_eemb, wembo, wei_hbm, weo_hbm, wni_hbm, wno_hbm, wgs, woh, wof,
               out0, out1,
               wei, weo, wni, wno, xst, xs, fm, g2m, m2g, glat, gcur, mlat, efl, ebase, elat, hsend, hin, hcur, hd,
               proj, recv, halo_s, halo_r, stage, wsh,
               wg, wemb, wg32, wemb32, w32, mis, msc, esc, gsnd, msnd, ghalo, mhalo, eft,
               wsem, xsem, sh_s, sh_r, osem, ef_s, ef_r, en_s, en_r, de_s, de_r, ha_s, ha_r):
        me = lax.axis_index("gp")
        left = lax.rem(me + group - 1, group)
        right = lax.rem(me + 1, group)
        blocks = 2 * group
        layers = wei_hbm.shape[0]

        barrier = pltpu.get_barrier_semaphore()
        for hop in range(1, group):
            pl.semaphore_signal(barrier, inc=1, device_id={"gp": lax.rem(me + hop, group)}, device_id_type=MESH_ID)

        weight_copies = [pltpu.make_async_copy(src, dst, wsem.at[i]) for i, (src, dst) in enumerate(
            [(wei_hbm, wei), (weo_hbm, weo), (wni_hbm, wni), (wno_hbm, wno)])]
        x_copies = [pltpu.make_async_copy(src, xst.at[i], xsem.at[i]) for i, src in enumerate((xc_hbm, xp_hbm))]
        for copy in x_copies:
            copy.start()
        for copy in weight_copies:
            copy.start()
        grid_dev = xst.shape[2]
        variables = xst.shape[1]
        half_grid = grid_dev // 2
        half_mesh = mesh_t.shape[1] // 2
        gsnd[0:g2m_t.shape[0], :] = g2m_t[:, 0:half_grid]
        msnd[0:mesh_t.shape[0], :] = mesh_t[:, 0:half_mesh]
        shift_copies = [pltpu.make_async_remote_copy(
            src_ref=src, dst_ref=dst, send_sem=sh_s.at[i], recv_sem=sh_r.at[i], device_id={"gp": left}, device_id_type=MESH_ID)
            for i, (src, dst) in enumerate(((gsnd, ghalo), (msnd, mhalo)))]

        mis[...] = jnp.zeros(mis.shape, F32)
        msc[...] = jnp.zeros(msc.shape, F32)
        esc[...] = jnp.zeros(esc.shape, F32)
        force = force_t.shape[0]
        for f in range(force):
            mis[8 * f:8 * f + 2, :] = force_t[f]
        mis[24:24 + static_t.shape[0], :] = static_t[...]
        mis[32:32 + m2g_t.shape[0], :] = m2g_t[...]
        mis[40:40 + g2m_t.shape[0], 0:half_grid] = g2m_t[:, half_grid:]
        msc[0:mesh_t.shape[0], 0:half_mesh] = mesh_t[:, half_mesh:]
        for k in range(6):
            esc[8 * k:8 * k + edge_t.shape[1], :] = edge_t[k]

        w32[0:w_grid.shape[0], :] = w_grid[...].astype(F32) * 0.5
        wg32[...] = jnp.zeros(wg32.shape, F32)
        wemb32[...] = jnp.zeros(wemb32.shape, F32)
        for s in range(2):
            wg32[s, 0:variables, :] = w32[0:variables, :]
            wg32[s, 128:128 + variables, :] = w32[variables:2 * variables, :]
            for f in range(force):
                wg32[s, 256 + 8 * f + s:257 + 8 * f + s, :] = w32[2 * variables + f:2 * variables + f + 1, :]
            for f in range(static_t.shape[0]):
                at = 2 * variables + force + f
                wg32[s, 280 + f:281 + f, :] = w32[at:at + 1, :]
            wg[s] = wg32[s].astype(BF16)
        places = [(40, w_eemb[0]), (32, w_eemb[1]), (0, w_mesh[...])] + [(8 * k, w_eemb[2]) for k in range(6)]
        for i, (at, rows) in enumerate(places):
            wemb32[i, at:at + rows.shape[0], :] = rows.astype(F32) * 0.5
            wemb[i] = wemb32[i].astype(BF16)

        def wide(rows):
            return jnp.concatenate([rows, jnp.zeros((128 - rows.shape[0], rows.shape[1]), F32)], axis=0).astype(BF16)

        for q in range(4):
            feats = dot_t(perms[2], wide(esc[:, q * 256:q * 256 + 256])).astype(BF16)
            for g in range(4):
                chunk = 4 * q + g
                eft[chunk // group, chunk % group] = feats[g * 64:g * 64 + 64]
        for slot in range(3):
            xs[slot] = jnp.zeros(xs.shape[1:], BF16)
        pl.semaphore_wait(barrier, group - 1)
        for copy in shift_copies:
            copy.start()

        def block_of(device, half):
            return lax.rem(2 * device + half, blocks)

        def ef_copy(hop, half):
            dest = lax.rem(me + hop, group)
            return pltpu.make_async_remote_copy(
                src_ref=eft.at[half, dest], dst_ref=efl.at[2 * me + half], send_sem=ef_s.at[dest, half],
                recv_sem=ef_r.at[me, half], device_id={"gp": dest}, device_id_type=MESH_ID)

        def ef_keep(half):
            return pltpu.make_async_copy(eft.at[half, me], efl.at[2 * me + half], ef_r.at[me, half])

        for half in range(2):
            for hop in range(1, group):
                ef_copy(hop, half).start()
            ef_keep(half).start()

        for copy in x_copies:
            copy.wait()
        mean = stats[:, 0:1]
        std = stats[:, 1:2]

        def embed_task(rows):
            misc = dot_t(perms[0], wide(mis[:, rows]))
            prev = dot_t(perms[0], ((xst[1, :, rows] - mean) / std).astype(BF16))
            cur = dot_t(perms[0], ((xst[0, :, rows] - mean) / std).astype(BF16))
            yield
            misc = misc.astype(BF16)
            fm[rows, :] = misc
            xs[0, rows, 0:variables] = prev.astype(BF16)
            xs[1, rows, 0:variables] = cur.astype(BF16)
            first = dot(misc, wemb[0])
            second = dot(misc, wemb[1])
            yield
            first = dot(silu_of_half(first), wembo[2])
            second = dot(silu_of_half(second), wembo[3])
            yield
            g2m[rows, :] = norm(first).astype(BF16)
            m2g[rows, :] = norm(second).astype(BF16)

        def embed_rows(it, carry):
            together(embed_task(pl.ds(pl.multiple_of((it * 4 + sub) * 256, 256), 256)) for sub in range(4))
            return carry

        lax.fori_loop(0, 2, embed_rows, 0)
        for copy in shift_copies:
            copy.wait_recv()
        mis[40:40 + g2m_t.shape[0], half_grid:] = ghalo[0:g2m_t.shape[0], :]
        msc[0:mesh_t.shape[0], half_mesh:] = mhalo[0:mesh_t.shape[0], :]
        lax.fori_loop(2, 4, embed_rows, 0)
        for copy in shift_copies:
            copy.wait_send()

        def plain_task(get, put, w_first, w_second):
            y = dot(get(), w_first)
            yield
            y = dot(silu_of_half(y), w_second)
            yield
            put(norm(y))

        def mesh_task(rows):
            def put(y):
                mlat[rows, :] = y.astype(BF16)
            feats = dot_t(perms[2], wide(msc[:, rows])).astype(BF16)
            return plain_task(lambda: feats, put, wemb[2], wembo[1])

        together(mesh_task(slice(sub * 256, sub * 256 + 256)) for sub in range(4))
        for copy in weight_copies:
            copy.wait()

        def halve(layer, carry):
            wei[layer] = wei[layer] * 0.5
            wni[layer] = wni[layer] * 0.5
            return carry

        lax.fori_loop(0, layers, halve, 0)
        wsh[0] = wgs[0] * 0.5
        wsh[1] = woh[...] * 0.5

        def en_copy(hop, half):
            dest = lax.rem(me + hop, group)
            return pltpu.make_async_remote_copy(
                src_ref=hsend.at[half, dest], dst_ref=hin.at[block_of(me, 1 + half)], send_sem=en_s.at[dest, half],
                recv_sem=en_r.at[me, half], device_id={"gp": dest}, device_id_type=MESH_ID)

        def de_copy(hop, half):
            dest = lax.rem(me + hop, group)
            return pltpu.make_async_remote_copy(
                src_ref=hcur.at[block_of(dest, 1 + half)], dst_ref=hd.at[half, me], send_sem=de_s.at[dest, half],
                recv_sem=de_r.at[me, half], device_id={"gp": dest}, device_id_type=MESH_ID)

        def en_arrival(source, half):
            return pltpu.make_async_remote_copy(
                src_ref=hsend.at[half, me], dst_ref=hin.at[block_of(source, 1 + half)], send_sem=en_s.at[me, half],
                recv_sem=en_r.at[source, half], device_id={"gp": left}, device_id_type=MESH_ID)

        def de_arrival(source, half):
            return pltpu.make_async_remote_copy(
                src_ref=hcur.at[0], dst_ref=hd.at[half, source], send_sem=de_s.at[me, half],
                recv_sem=de_r.at[source, half], device_id={"gp": left}, device_id_type=MESH_ID)

        def ef_arrival(source, half):
            return pltpu.make_async_remote_copy(
                src_ref=eft.at[half, me], dst_ref=efl.at[2 * source + half], send_sem=ef_s.at[me, half],
                recv_sem=ef_r.at[source, half], device_id={"gp": left}, device_id_type=MESH_ID)

        def halo_copies(slot):
            return [pltpu.make_async_remote_copy(
                src_ref=halo_s.at[slot, side], dst_ref=halo_r.at[slot, 1 - side], send_sem=ha_s.at[slot, side],
                recv_sem=ha_r.at[slot, 1 - side], device_id={"gp": (left, right)[side]}, device_id_type=MESH_ID)
                for side in range(2)]

        def send_halo(slot):
            for b in range(blocks):
                stage[0, b:b + 1, :] = hcur[b, 0:16, :].astype(F32)[0:1]
                stage[1, b:b + 1, :] = hcur[b, 48:64, :].astype(F32)[15:16]
            halo_s[slot, 0] = stage[0].astype(BF16)
            halo_s[slot, 1] = stage[1].astype(BF16)
            for copy in halo_copies(slot):
                copy.start()

        def edge_task(layer, k, sub, size, send):
            rows = slice(sub, sub + size)
            old = elat[k, rows, :]
            pre = dot(old, wei[layer, 0:256, :]) + (send + recv[rows, :])
            yield
            y = dot(silu_of_half(pre), weo[layer])
            yield
            elat[k, rows, :] = residual(old, norm(y))

        def project(layer, lo, hi):
            h = hcur[lo:hi].reshape((hi - lo) * 64, 256)
            return dot(h, wei[layer, 256:512, :]), dot(h, wei[layer, 512:768, :])

        def put_projections(lo, hi, send, receive):
            proj[lo:hi, 8:72, :] = send.reshape(hi - lo, 64, 256)
            recv[lo * 64:hi * 64, :] = receive

        def tail_task(layer, lo, hi):
            size = (hi - lo) * 64
            rows = slice(lo * 64, hi * 64)
            olds = [elat[k, rows, :] for k in range(2)]
            sends = [proj[lo:hi, 16:80, :].reshape(size, 256), proj[lo:hi, 0:64, :].reshape(size, 256)]
            pres = [dot(old, wei[layer, 0:256, :]) + (send + recv[rows, :]) for old, send in zip(olds, sends)]
            total = elat[2, rows, :].astype(F32)
            for k in range(3, 6):
                total = total + elat[k, rows, :].astype(F32)
            yield
            ys = [dot(silu_of_half(pre), weo[layer]) for pre in pres]
            yield
            for k in range(2):
                new = residual(olds[k], norm(ys[k]))
                elat[k, rows, :] = new
                total = total + new.astype(F32)
            node = hcur[lo:hi].reshape(size, 256)
            pre = dot(node, wni[layer, 0:256, :]) + dot(total.astype(BF16), wni[layer, 256:512, :])
            yield
            y = dot(silu_of_half(pre), wno[layer])
            yield
            new = residual(node, norm(y))
            hcur[lo:hi] = new.reshape(hi - lo, 64, 256)
            send = dot(new, wei[layer + 1, 256:512, :])
            receive = dot(new, wei[layer + 1, 512:768, :])
            yield
            put_projections(lo, hi, send, receive)

        def rolled(shift, sub, size):
            lo, count = sub // 64, size // 64
            picks = [(lo + q + shift) % blocks for q in range(count)]
            return jnp.concatenate([proj[b, 8:72, :] for b in picks], axis=0)

        def mesh_layer(layer, carry):
            slot = lax.rem(layer, 2)
            staggered((edge_task(layer, k, sub, SUB, rolled(shift, sub, SUB))
                       for k, shift in ((2, 1), (3, -1), (4, 4), (5, -4)) for sub in range(0, blocks * 64, SUB)), WIDTH)
            for copy in halo_copies(slot):
                copy.wait_recv()
            for copy in halo_copies(slot):
                copy.wait_send()
            edge_proj = dot(halo_r[slot].reshape(32, 256), wei[layer, 256:512, :])
            low = edge_proj[0:16]
            high = edge_proj[16:32]
            stage[0] = jnp.where(me == 0, jnp.concatenate([low[15:16], low[0:15]], axis=0), low)
            stage[1] = jnp.where(me == group - 1, jnp.concatenate([high[1:16], high[0:1]], axis=0), high)
            sublane = lax.broadcasted_iota(jnp.int32, (8, 256), 0)
            for b in range(blocks):
                proj[b, 0:8, :] = jnp.where(sublane == 0, stage[0, b:b + 1, :], pltpu.roll(proj[b, 64:72, :], 1, 0))
                proj[b, 72:80, :] = jnp.where(sublane == 7, stage[1, b:b + 1, :], pltpu.roll(proj[b, 8:16, :], 7, 0))
            staggered((tail_task(layer, lo, lo + TAIL // 64) for lo in range(0, blocks, TAIL // 64)), TAIL_WIDTH)

            @pl.when(layer < layers - 2)
            def _():
                send_halo(1 - slot)
            return carry

        def forecast(step, carry):
            def encode_task(dest, half):
                chunk = half * group + dest
                rows = pl.ds(pl.multiple_of(chunk * 256, 256), 256)
                feats = jnp.concatenate([xs[step, rows, :], xs[step + 1, rows, :]], axis=1)
                node = mlat[pl.ds(pl.multiple_of(chunk * 64, 64), 64), :]
                old = g2m[rows, :]
                pre = dot(feats, wg[step, 0:256, :]) + dot(fm[rows, :], wg[step, 256:384, :])
                yield
                y = dot(silu_of_half(pre), wembo[0])
                yield
                lat = norm(y).astype(BF16)
                glat[rows, :] = lat
                pre = dot(old, wei[0, 0:256, :]) + dot(lat, wei[0, 256:512, :])
                term = dot(node, wei[0, 512:768, :])
                yield
                pre = pre + jnp.concatenate([term] * 4, axis=0)
                y = dot(silu_of_half(pre), weo[0])
                yield
                edge = residual(old, norm(y)).astype(F32)
                return node, (edge[0:64] + edge[64:128] + edge[128:192] + edge[192:256]).astype(BF16)

            def encode_group(pairs):
                results = []

                def run(dest, half):
                    results.append((yield from encode_task(dest, half)))

                active = [run(dest, half) for dest, half in pairs]
                while active:
                    active = [task for task in active if next(task, "done") != "done"]
                    yield
                node = jnp.concatenate([r[0] for r in results], axis=0)
                esum = jnp.concatenate([r[1] for r in results], axis=0)
                pre = dot(node, wni[0, 0:256, :]) + dot(esum, wni[0, 256:512, :])
                yield
                y = dot(silu_of_half(pre), wno[0])
                yield
                new = residual(node, norm(y))
                for q, (dest, half) in enumerate(pairs):
                    hsend[half, dest] = new[q * 64:q * 64 + 64]

            def encode(it, carry):
                dests = [lax.rem(me + PER * it + 1 + q, group) for q in range(PER)]
                pairs = [(dest, half) for dest in dests for half in range(2)]
                staggered((encode_group(pairs[lo:lo + 4]) for lo in range(0, 2 * PER, 4)), 4)
                for q in range(PER - 1):
                    for half in range(2):
                        en_copy(PER * it + 1 + q, half).start()

                @pl.when(it < group // PER - 1)
                def _():
                    for half in range(2):
                        en_copy(PER * it + PER, half).start()
                return carry

            lax.fori_loop(0, group // PER, encode, 0)

            @pl.when(step == 0)
            def _():
                for half in range(2):
                    for hop in range(1, group):
                        ef_arrival(lax.rem(me + hop, group), half).wait_recv()
                    ef_keep(half).wait()

                def embed_edges(k, carry):
                    def edge_embed_task(sub):
                        def put(y):
                            ebase[k, sub * 64:sub * 64 + 256, :] = y.astype(BF16)
                        return plain_task(lambda: efl[sub:sub + 4].reshape(256, 128), put, wemb[3 + k], wembo[4])

                    together(edge_embed_task(sub) for sub in range(0, blocks, 4))
                    return carry

                lax.fori_loop(0, 6, embed_edges, 0)
                for hop in range(1, group):
                    for half in range(2):
                        ef_copy(hop, half).wait_send()

            elat[...] = ebase[...]
            for hop in range(1, group):
                for half in range(2):
                    en_arrival(lax.rem(me + hop, group), half).wait_recv()
            for hop in range(1, group):
                for half in range(2):
                    en_copy(hop, half).wait_send()
            hcur[...] = hin[...]
            for half in range(2):
                hcur[block_of(me, 1 + half)] = hsend[half, me]
            send_halo(1)
            put_projections(0, blocks, *project(1, 0, blocks))
            lax.fori_loop(1, layers - 1, mesh_layer, 0)
            for hop in range(1, group):
                for half in range(2):
                    de_copy(hop, half).start()
            for half in range(2):
                hd[half, me] = hcur[block_of(me, 1 + half)]

            def self_task(rows):
                old = glat[rows, :]

                def put(y):
                    gcur[rows, :] = residual(old, y)
                return plain_task(lambda: old, put, wsh[0], wgs[1])

            def self_update(it, carry):
                together(self_task(pl.ds(pl.multiple_of((it * 4 + sub) * 256, 256), 256)) for sub in range(4))
                return carry

            lax.fori_loop(0, 4, self_update, 0)

            def decode(it, carry):
                last = layers - 1
                for q in range(PER - 1):
                    for half in range(2):
                        de_arrival(lax.rem(me + PER * it + 1 + q, group), half).wait_recv()

                @pl.when(it < group // PER - 1)
                def _():
                    for half in range(2):
                        de_arrival(lax.rem(me + PER * it + PER, group), half).wait_recv()

                work = []
                for q in range(PER):
                    source = lax.rem(me + PER * it + 1 + q, group)
                    for half in range(2):
                        rows = pl.ds(pl.multiple_of((half * group + source) * 256, 256), 256)
                        work.append((rows, hd[half, source], m2g[rows, :], gcur[rows, :], xst[step, :, rows]))
                def decode_task(rows, node, old, grid, state):
                    pre = dot(old, wei[last, 0:256, :]) + dot(grid, wei[last, 512:768, :])
                    term = dot(node, wei[last, 256:512, :])
                    yield
                    pre = pre + jnp.concatenate([term] * 4, axis=0)
                    y = dot(silu_of_half(pre), weo[last])
                    yield
                    edge = residual(old, norm(y))
                    pre = dot(grid, wni[last, 0:256, :]) + dot(edge, wni[last, 256:512, :])
                    yield
                    y = dot(silu_of_half(pre), wno[last])
                    yield
                    out = residual(grid, norm(y))
                    pre = dot(out, wsh[1])
                    yield
                    hidden = dot(perms[1], silu_of_half(pre))
                    yield
                    p = dot_t(wof[...], hidden.astype(BF16))
                    yield
                    new = state + stats[:, 3:4] * p + stats[:, 2:3]
                    scaled = dot_t(perms[0], ((new - mean) / std).astype(BF16))
                    yield
                    xst[step + 1, :, rows] = new
                    xs[2, rows, 0:variables] = scaled.astype(BF16)

                staggered((decode_task(*args) for args in work), 2 * PER)
                return carry

            lax.fori_loop(0, group // PER, decode, 0)
            for hop in range(1, group):
                for half in range(2):
                    de_copy(hop, half).wait_send()

            @pl.when(step == 0)
            def _():
                pltpu.make_async_copy(xst.at[1], out0, osem.at[0]).start()
            return carry

        lax.fori_loop(0, 2, forecast, 0)
        final = pltpu.make_async_copy(xst.at[2], out1, osem.at[1])
        final.start()
        pltpu.make_async_copy(xst.at[1], out0, osem.at[0]).wait()
        final.wait()

    def local_run(x_prev, x_cur, forcing, grid_static, g2m_feat, m2g_feat, mesh_feat, mesh_edge_feat, norm_stats, w_grid_in, w_mesh_in, w_eemb_in, w_embed_out, w_edge_in, w_edge_out, w_node_in, w_node_out, w_grid_self, w_out_hidden, w_out_final):
        grid_dev, variables = x_prev.shape
        mesh_dev = mesh_feat.shape[0]
        latent = w_embed_out.shape[-1]
        blocks = 2 * group
        perms = jnp.asarray(row_permutation(), BF16)

        vmem = pl.BlockSpec(memory_space=pltpu.VMEM)
        anywhere = pl.BlockSpec(memory_space=pl.ANY)
        state = jax.ShapeDtypeStruct((variables, grid_dev), F32)
        dma = pltpu.SemaphoreType.DMA
        first, second = pl.pallas_call(
            kernel,
            out_shape=(state, state),
            in_specs=[anywhere, anywhere] + [vmem] * 12 + [anywhere] * 4 + [vmem] * 3,
            out_specs=(anywhere, anywhere),
            scratch_shapes=[
                pltpu.VMEM(w_edge_in.shape, BF16), pltpu.VMEM(w_edge_out.shape, BF16),
                pltpu.VMEM(w_node_in.shape, BF16), pltpu.VMEM(w_node_out.shape, BF16),
                pltpu.VMEM((3, variables, grid_dev), F32), pltpu.VMEM((3, grid_dev, 128), BF16), pltpu.VMEM((grid_dev, 128), BF16),
                pltpu.VMEM((grid_dev, latent), BF16), pltpu.VMEM((grid_dev, latent), BF16), pltpu.VMEM((grid_dev, latent), BF16),
                pltpu.VMEM((grid_dev, latent), BF16),
                pltpu.VMEM((mesh_dev, latent), BF16), pltpu.VMEM((blocks, 64, 128), BF16),
                pltpu.VMEM((6, mesh_dev, latent), BF16), pltpu.VMEM((6, mesh_dev, latent), BF16),
                pltpu.VMEM((2, group, 64, latent), BF16), pltpu.VMEM((blocks, 64, latent), BF16),
                pltpu.VMEM((blocks, 64, latent), BF16), pltpu.VMEM((2, group, 64, latent), BF16),
                pltpu.VMEM((blocks, 80, latent), F32), pltpu.VMEM((mesh_dev, latent), F32),
                pltpu.VMEM((2, 2, blocks, latent), BF16), pltpu.VMEM((2, 2, blocks, latent), BF16), pltpu.VMEM((2, blocks, latent), F32), pltpu.VMEM((2, latent, latent), BF16),
                pltpu.VMEM((2, 384, latent), BF16), pltpu.VMEM((9, 128, latent), BF16), pltpu.VMEM((2, 384, latent), F32),
                pltpu.VMEM((9, 128, latent), F32), pltpu.VMEM((-(-w_grid_in.shape[0] // 8) * 8, latent), F32),
                pltpu.VMEM((64, grid_dev), F32), pltpu.VMEM((8, mesh_dev), F32), pltpu.VMEM((48, mesh_dev), F32),
                pltpu.VMEM((8, grid_dev // 2), F32), pltpu.VMEM((8, mesh_dev // 2), F32), pltpu.VMEM((8, grid_dev // 2), F32),
                pltpu.VMEM((8, mesh_dev // 2), F32), pltpu.VMEM((2, group, 64, 128), BF16),
                dma((4,)), dma((2,)), dma((2,)), dma((2,)), dma((2,)), dma((group, 2)), dma((group, 2)), dma((group, 2)), dma((group, 2)),
                dma((group, 2)), dma((group, 2)), dma((2, 2)), dma((2, 2)),
            ],
            compiler_params=pltpu.CompilerParams(collective_id=0, has_side_effects=True, flags=FLAGS, vmem_limit_bytes=67043328),
        )(x_prev.T, x_cur.T, forcing.transpose(2, 1, 0), grid_static.T, g2m_feat.T, m2g_feat.T, mesh_feat.T, mesh_edge_feat.transpose(1, 2, 0),
          norm_stats.T, perms, w_grid_in, w_mesh_in, w_eemb_in, w_embed_out, w_edge_in, w_edge_out, w_node_in, w_node_out, w_grid_self,
          w_out_hidden, w_out_final.T)
        return first.T, second.T

    row_spec = P(("dp", "gp"))
    edge_spec = P(("dp", "gp"), None, None)
    whole = P()
    in_specs = (row_spec, row_spec, edge_spec, row_spec, row_spec, row_spec, row_spec, edge_spec, whole) + (whole,) * 11
    return jax.shard_map(local_run, mesh=mesh, in_specs=in_specs, out_specs=(row_spec, row_spec), check_vma=False)
```

```python
import jax
import jax.numpy as jnp
import numpy as np
from jax import lax
from jax.experimental import pallas as pl
from jax.experimental.pallas import tpu as pltpu
from jax.sharding import PartitionSpec as P

MESH_ID = pl.DeviceIdType.MESH
F32 = jnp.float32
BF16 = jnp.bfloat16
SUB = 256
PER = 4
WIDTH = 3
TAIL_WIDTH = 6
FLAGS = {}


def dot(a, b):
    return jnp.dot(a, b, preferred_element_type=F32)


def dot_t(a, b):
    return lax.dot_general(a, b, (((1,), (1,)), ((), ())), preferred_element_type=F32)


def silu_of_half(half):
    return (half * jnp.tanh(half) + half).astype(BF16)


def norm(y):
    z = y - jnp.mean(y, axis=-1, keepdims=True)
    return z * lax.rsqrt(jnp.mean(z * z, axis=-1, keepdims=True) + 1e-5)


def staggered(tasks, width):
    waiting = list(tasks)
    active = []
    while waiting or active:
        if waiting and len(active) < width:
            active.append(waiting.pop(0))
        for task in list(active):
            if next(task, "done") == "done":
                active.remove(task)


def together(tasks):
    active = list(tasks)
    while active:
        active = [task for task in active if next(task, "done") != "done"]


def residual(base, update):
    return (base.astype(F32) + update).astype(BF16)


def row_permutation():
    perm = np.zeros((256, 256), np.float32)
    for r in range(4):
        for j in range(8):
            for i in range(8):
                perm[r * 64 + j * 8 + i, (i * 8 + j) * 4 + r] = 1.0
    swap = np.zeros((256, 256), np.float32)
    for g in range(4):
        for j in range(8):
            for i in range(8):
                swap[g * 64 + j * 8 + i, g * 64 + i * 8 + j] = 1.0
    return np.stack([perm, perm.T, swap])


def solution(mesh):
    group = mesh.shape["gp"]

    def kernel(xp_hbm, xc_hbm, force_t, static_t, g2m_t, m2g_t, mesh_t, edge_t, stats, perms, w_grid, w_mesh, w_eemb, wembo, wei_hbm, weo_hbm, wni_hbm, wno_hbm, wgs, woh, wof,
               out0, out1,
               wei, weo, wni, wno, xst, xs, fm, g2m, m2g, glat, gcur, mlat, efl, ebase, elat, hsend, hin, hcur, hd,
               proj, recv, halo_s, halo_r, stage, wsh, hb, efj,
               wg, wemb, wg32, wemb32, w32, mis, msc, esc, gsnd, msnd, ghalo, mhalo, eft,
               wsem, xsem, sh_s, sh_r, osem, ef_s, ef_r, en_s, en_r, de_s, de_r, ha_s, ha_r):
        me = lax.axis_index("gp")
        left = lax.rem(me + group - 1, group)
        right = lax.rem(me + 1, group)
        blocks = 2 * group
        layers = wei_hbm.shape[0]

        barrier = pltpu.get_barrier_semaphore()
        for hop in range(1, group):
            pl.semaphore_signal(barrier, inc=1, device_id={"gp": lax.rem(me + hop, group)}, device_id_type=MESH_ID)

        weight_copies = [pltpu.make_async_copy(src, dst, wsem.at[i]) for i, (src, dst) in enumerate(
            [(wei_hbm, wei), (weo_hbm, weo), (wni_hbm, wni), (wno_hbm, wno)])]
        x_copies = [pltpu.make_async_copy(src, xst.at[i], xsem.at[i]) for i, src in enumerate((xc_hbm, xp_hbm))]
        for copy in x_copies:
            copy.start()
        for copy in weight_copies:
            copy.start()
        grid_dev = xst.shape[2]
        variables = xst.shape[1]
        half_grid = grid_dev // 2
        half_mesh = mesh_t.shape[1] // 2
        gsnd[0:g2m_t.shape[0], :] = g2m_t[:, 0:half_grid]
        msnd[0:mesh_t.shape[0], :] = mesh_t[:, 0:half_mesh]
        shift_copies = [pltpu.make_async_remote_copy(
            src_ref=src, dst_ref=dst, send_sem=sh_s.at[i], recv_sem=sh_r.at[i], device_id={"gp": left}, device_id_type=MESH_ID)
            for i, (src, dst) in enumerate(((gsnd, ghalo), (msnd, mhalo)))]

        mis[...] = jnp.zeros(mis.shape, F32)
        msc[...] = jnp.zeros(msc.shape, F32)
        esc[...] = jnp.zeros(esc.shape, F32)
        force = force_t.shape[0]
        for f in range(force):
            mis[8 * f:8 * f + 2, :] = force_t[f]
        mis[24:24 + static_t.shape[0], :] = static_t[...]
        mis[32:32 + m2g_t.shape[0], :] = m2g_t[...]
        mis[40:40 + g2m_t.shape[0], 0:half_grid] = g2m_t[:, half_grid:]
        msc[0:mesh_t.shape[0], 0:half_mesh] = mesh_t[:, half_mesh:]
        for k in range(6):
            esc[8 * k:8 * k + edge_t.shape[1], :] = edge_t[k]

        w32[0:w_grid.shape[0], :] = w_grid[...].astype(F32) * 0.5
        wg32[...] = jnp.zeros(wg32.shape, F32)
        wemb32[...] = jnp.zeros(wemb32.shape, F32)
        for s in range(2):
            wg32[s, 0:variables, :] = w32[0:variables, :]
            wg32[s, 128:128 + variables, :] = w32[variables:2 * variables, :]
            for f in range(force):
                wg32[s, 256 + 8 * f + s:257 + 8 * f + s, :] = w32[2 * variables + f:2 * variables + f + 1, :]
            for f in range(static_t.shape[0]):
                at = 2 * variables + force + f
                wg32[s, 280 + f:281 + f, :] = w32[at:at + 1, :]
            wg[s] = wg32[s].astype(BF16)
        places = [(40, w_eemb[0]), (32, w_eemb[1]), (0, w_mesh[...])] + [(8 * k, w_eemb[2]) for k in range(6)]
        for i, (at, rows) in enumerate(places):
            wemb32[i, at:at + rows.shape[0], :] = rows.astype(F32) * 0.5
            wemb[i] = wemb32[i].astype(BF16)

        def wide(rows):
            return jnp.concatenate([rows, jnp.zeros((128 - rows.shape[0], rows.shape[1]), F32)], axis=0).astype(BF16)

        for q in range(4):
            feats = dot_t(perms[2], wide(esc[:, q * 256:q * 256 + 256])).astype(BF16)
            for g in range(4):
                chunk = 4 * q + g
                eft[chunk // group, chunk % group] = feats[g * 64:g * 64 + 64]
        for slot in range(3):
            xs[slot] = jnp.zeros(xs.shape[1:], BF16)
        pl.semaphore_wait(barrier, group - 1)
        for copy in shift_copies:
            copy.start()

        def block_of(device, half):
            return lax.rem(2 * device + half, blocks)

        def ef_copy(hop, half):
            dest = lax.rem(me + hop, group)
            return pltpu.make_async_remote_copy(
                src_ref=eft.at[half, dest], dst_ref=efl.at[2 * me + half], send_sem=ef_s.at[dest, half],
                recv_sem=ef_r.at[me, half], device_id={"gp": dest}, device_id_type=MESH_ID)

        def ef_keep(half):
            return pltpu.make_async_copy(eft.at[half, me], efl.at[2 * me + half], ef_r.at[me, half])

        for half in range(2):
            for hop in range(1, group):
                ef_copy(hop, half).start()
            ef_keep(half).start()

        for copy in x_copies:
            copy.wait()
        mean = stats[:, 0:1]
        std = stats[:, 1:2]

        def embed_task(rows):
            misc = dot_t(perms[0], wide(mis[:, rows]))
            prev = dot_t(perms[0], ((xst[1, :, rows] - mean) / std).astype(BF16))
            cur = dot_t(perms[0], ((xst[0, :, rows] - mean) / std).astype(BF16))
            yield
            misc = misc.astype(BF16)
            fm[rows, :] = misc
            xs[0, rows, 0:variables] = prev.astype(BF16)
            xs[1, rows, 0:variables] = cur.astype(BF16)
            first = dot(misc, wemb[0])
            second = dot(misc, wemb[1])
            yield
            first = dot(silu_of_half(first), wembo[2])
            second = dot(silu_of_half(second), wembo[3])
            yield
            g2m[rows, :] = norm(first).astype(BF16)
            m2g[rows, :] = norm(second).astype(BF16)

        def embed_rows(it, carry):
            together(embed_task(pl.ds(pl.multiple_of((it * 4 + sub) * 256, 256), 256)) for sub in range(4))
            return carry

        lax.fori_loop(0, 2, embed_rows, 0)
        for copy in shift_copies:
            copy.wait_recv()
        mis[40:40 + g2m_t.shape[0], half_grid:] = ghalo[0:g2m_t.shape[0], :]
        msc[0:mesh_t.shape[0], half_mesh:] = mhalo[0:mesh_t.shape[0], :]
        lax.fori_loop(2, 4, embed_rows, 0)
        for copy in shift_copies:
            copy.wait_send()

        def plain_task(get, put, w_first, w_second):
            y = dot(get(), w_first)
            yield
            y = dot(silu_of_half(y), w_second)
            yield
            put(norm(y))

        def mesh_task(rows):
            def put(y):
                mlat[rows, :] = y.astype(BF16)
            feats = dot_t(perms[2], wide(msc[:, rows])).astype(BF16)
            return plain_task(lambda: feats, put, wemb[2], wembo[1])

        together(mesh_task(slice(sub * 256, sub * 256 + 256)) for sub in range(4))
        for copy in weight_copies:
            copy.wait()

        def halve(layer, carry):
            wei[layer] = wei[layer] * 0.5
            wni[layer] = wni[layer] * 0.5
            return carry

        lax.fori_loop(0, layers, halve, 0)
        wsh[0] = wgs[0] * 0.5
        wsh[1] = woh[...] * 0.5

        def en_copy(hop, half):
            dest = lax.rem(me + hop, group)
            return pltpu.make_async_remote_copy(
                src_ref=hsend.at[half, dest], dst_ref=hin.at[block_of(me, 1 + half)], send_sem=en_s.at[dest, half],
                recv_sem=en_r.at[me, half], device_id={"gp": dest}, device_id_type=MESH_ID)

        def de_copy(hop, half):
            dest = lax.rem(me + hop, group)
            return pltpu.make_async_remote_copy(
                src_ref=hb.at[block_of(dest, 1 + half)], dst_ref=hd.at[half, me], send_sem=de_s.at[dest, half],
                recv_sem=de_r.at[me, half], device_id={"gp": dest}, device_id_type=MESH_ID)

        def en_arrival(source, half):
            return pltpu.make_async_remote_copy(
                src_ref=hsend.at[half, me], dst_ref=hin.at[block_of(source, 1 + half)], send_sem=en_s.at[me, half],
                recv_sem=en_r.at[source, half], device_id={"gp": left}, device_id_type=MESH_ID)

        def de_arrival(source, half):
            return pltpu.make_async_remote_copy(
                src_ref=hb.at[0], dst_ref=hd.at[half, source], send_sem=de_s.at[me, half],
                recv_sem=de_r.at[source, half], device_id={"gp": left}, device_id_type=MESH_ID)

        def ef_arrival(source, half):
            return pltpu.make_async_remote_copy(
                src_ref=eft.at[half, me], dst_ref=efl.at[2 * source + half], send_sem=ef_s.at[me, half],
                recv_sem=ef_r.at[source, half], device_id={"gp": left}, device_id_type=MESH_ID)

        def halo_copy(slot, side):
            return pltpu.make_async_remote_copy(
                src_ref=halo_s.at[slot, side], dst_ref=halo_r.at[slot, 1 - side], send_sem=ha_s.at[slot, side],
                recv_sem=ha_r.at[slot, 1 - side], device_id={"gp": (left, right)[side]}, device_id_type=MESH_ID)

        def wait_halo(slot):
            for side in range(2):
                halo_copy(slot, 1 - side).wait_recv()
            for side in range(2):
                halo_copy(slot, side).wait_send()

        def send_halo(slot, side, rows):
            for b in range(blocks):
                at = 8 * b + 7 * side
                stage[2 + side, b:b + 1, :] = rows[at:at + 1]
            halo_s[slot, side] = stage[2 + side].astype(BF16)
            halo_copy(slot, side).start()

        def by_j(values):
            return jnp.concatenate([values[:, 8 * j:8 * j + 8, :].reshape(blocks * 8, values.shape[-1]) for j in range(8)], axis=0)

        def by_block(values):
            values = values.reshape(8, blocks, 8, values.shape[-1])
            return jnp.stack([values[:, b].reshape(64, values.shape[-1]) for b in range(blocks)], axis=0)

        span = blocks * 8

        def rolled(shift, sub, size):
            cut = shift % blocks * 8
            pieces = []
            for base in range(sub + span, sub + size + span, span):
                pieces += [proj[base + cut:base + span, :], proj[base:base + cut, :]]
            return jnp.concatenate(pieces, axis=0)

        def edge_send(k, sub, size):
            if k == 0:
                return proj[sub + 2 * span:sub + 2 * span + size, :]
            if k == 1:
                return proj[sub:sub + size, :]
            return rolled((1, -1, 4, -4)[k - 2], sub, size)

        def edge_task(layer, k, sub, size):
            rows = slice(sub, sub + size)
            old = elat[k, rows, :]
            pre = dot(old, wei[layer, 0:256, :]) + (edge_send(k, sub, size) + recv[rows, :])
            yield
            y = dot(silu_of_half(pre), weo[layer])
            yield
            elat[k, rows, :] = residual(old, norm(y))

        def put_projections(rows, send, receive):
            proj[rows.start + span:rows.stop + span, :] = send
            recv[rows, :] = receive

        def node_task(layer, sub, size):
            rows = slice(sub, sub + size)
            total = elat[0, rows, :].astype(F32)
            for k in range(1, 6):
                total = total + elat[k, rows, :].astype(F32)
            node = hcur[rows, :]
            pre = dot(node, wni[layer, 0:256, :]) + dot(total.astype(BF16), wni[layer, 256:512, :])
            yield
            y = dot(silu_of_half(pre), wno[layer])
            yield
            new = residual(node, norm(y))
            hcur[rows, :] = new
            send = dot(new, wei[layer + 1, 256:512, :])
            receive = dot(new, wei[layer + 1, 512:768, :])
            next_slot = lax.rem(layer + 1, 2)
            if sub == 0:
                send_halo(next_slot, 0, new[0:span].astype(F32))
            if sub + size == 8 * span:
                send_halo(next_slot, 1, new[size - span:size].astype(F32))
            yield
            put_projections(rows, send, receive)

        def mesh_layer(layer, carry):
            slot = lax.rem(layer, 2)
            for b in range(blocks):
                proj[8 * b:8 * b + 8, :] = pltpu.roll(proj[8 * span + 8 * b:8 * span + 8 * b + 8, :], 1, 0)
                proj[9 * span + 8 * b:9 * span + 8 * b + 8, :] = pltpu.roll(proj[span + 8 * b:span + 8 * b + 8, :], 7, 0)
            size = 2 * span
            subs = range(0, 8 * span, size)
            early = [(k, sub) for k in (2, 3, 4, 5) for sub in subs]
            early += [(0, sub) for sub in subs[:-1]] + [(1, sub) for sub in subs[1:]]
            staggered((edge_task(layer, k, sub, size) for k, sub in early), WIDTH)
            wait_halo(slot)
            edge_proj = dot(halo_r[slot].reshape(2 * blocks, 256), wei[layer, 256:512, :])
            low = edge_proj[0:blocks]
            high = edge_proj[blocks:2 * blocks]
            stage[0] = jnp.where(me == 0, jnp.concatenate([low[blocks - 1:], low[:blocks - 1]], axis=0), low)
            stage[1] = jnp.where(me == group - 1, jnp.concatenate([high[1:], high[:1]], axis=0), high)
            for b in range(blocks):
                proj[8 * b:8 * b + 1, :] = stage[0, b:b + 1, :]
                proj[9 * span + 8 * b + 7:9 * span + 8 * b + 8, :] = stage[1, b:b + 1, :]
            tasks = [edge_task(layer, 1, 0, size), edge_task(layer, 0, subs[-1], size)]
            tasks += [node_task(layer, sub, size) for sub in (subs[1], subs[0], subs[-1], subs[2])]
            staggered(tasks, TAIL_WIDTH)
            return carry

        def forecast(step, carry):
            def encode_task(dest, half):
                chunk = half * group + dest
                rows = pl.ds(pl.multiple_of(chunk * 256, 256), 256)
                feats = jnp.concatenate([xs[step, rows, :], xs[step + 1, rows, :]], axis=1)
                node = mlat[pl.ds(pl.multiple_of(chunk * 64, 64), 64), :]
                old = g2m[rows, :]
                pre = dot(feats, wg[step, 0:256, :]) + dot(fm[rows, :], wg[step, 256:384, :])
                yield
                y = dot(silu_of_half(pre), wembo[0])
                yield
                lat = norm(y).astype(BF16)
                glat[rows, :] = lat
                pre = dot(old, wei[0, 0:256, :]) + dot(lat, wei[0, 256:512, :])
                term = dot(node, wei[0, 512:768, :])
                yield
                pre = pre + jnp.concatenate([term] * 4, axis=0)
                y = dot(silu_of_half(pre), weo[0])
                yield
                edge = residual(old, norm(y)).astype(F32)
                return node, (edge[0:64] + edge[64:128] + edge[128:192] + edge[192:256]).astype(BF16)

            def encode_group(pairs):
                results = []

                def run(dest, half):
                    results.append((yield from encode_task(dest, half)))

                active = [run(dest, half) for dest, half in pairs]
                while active:
                    active = [task for task in active if next(task, "done") != "done"]
                    yield
                node = jnp.concatenate([r[0] for r in results], axis=0)
                esum = jnp.concatenate([r[1] for r in results], axis=0)
                pre = dot(node, wni[0, 0:256, :]) + dot(esum, wni[0, 256:512, :])
                yield
                y = dot(silu_of_half(pre), wno[0])
                yield
                new = residual(node, norm(y))
                for q, (dest, half) in enumerate(pairs):
                    hsend[half, dest] = new[q * 64:q * 64 + 64]

            def encode(it, carry):
                dests = [lax.rem(me + PER * it + 1 + q, group) for q in range(PER)]
                pairs = [(dest, half) for dest in dests for half in range(2)]
                staggered((encode_group(pairs[lo:lo + 4]) for lo in range(0, 2 * PER, 4)), 4)
                for q in range(PER - 1):
                    for half in range(2):
                        en_copy(PER * it + 1 + q, half).start()

                @pl.when(it < group // PER - 1)
                def _():
                    for half in range(2):
                        en_copy(PER * it + PER, half).start()
                return carry

            lax.fori_loop(0, group // PER, encode, 0)

            @pl.when(step == 0)
            def _():
                for half in range(2):
                    for hop in range(1, group):
                        ef_arrival(lax.rem(me + hop, group), half).wait_recv()
                    ef_keep(half).wait()

                efj[...] = by_j(efl[...].astype(F32)).astype(BF16)

                def embed_edges(k, carry):
                    def edge_embed_task(sub):
                        def put(y):
                            ebase[k, sub * 64:sub * 64 + 256, :] = y.astype(BF16)
                        return plain_task(lambda: efj[sub * 64:sub * 64 + 256, :], put, wemb[3 + k], wembo[4])

                    together(edge_embed_task(sub) for sub in range(0, blocks, 4))
                    return carry

                lax.fori_loop(0, 6, embed_edges, 0)
                for hop in range(1, group):
                    for half in range(2):
                        ef_copy(hop, half).wait_send()

            elat[...] = ebase[...]
            for hop in range(1, group):
                for half in range(2):
                    en_arrival(lax.rem(me + hop, group), half).wait_recv()
            for hop in range(1, group):
                for half in range(2):
                    en_copy(hop, half).wait_send()
            for half in range(2):
                hin[block_of(me, 1 + half)] = hsend[half, me]
            start = by_j(hin[...].astype(F32))
            send_halo(1, 0, start[0:span])
            send_halo(1, 1, start[7 * span:])
            start = start.astype(BF16)
            hcur[...] = start
            put_projections(slice(0, 8 * span), dot(start, wei[1, 256:512, :]), dot(start, wei[1, 512:768, :]))
            lax.fori_loop(1, layers - 1, mesh_layer, 0)
            hb[...] = by_block(hcur[...].astype(F32)).astype(BF16)
            for hop in range(1, group):
                for half in range(2):
                    de_copy(hop, half).start()
            for half in range(2):
                hd[half, me] = hb[block_of(me, 1 + half)]

            def self_task(rows):
                old = glat[rows, :]

                def put(y):
                    gcur[rows, :] = residual(old, y)
                return plain_task(lambda: old, put, wsh[0], wgs[1])

            def self_update(it, carry):
                together(self_task(pl.ds(pl.multiple_of((it * 4 + sub) * 256, 256), 256)) for sub in range(4))
                return carry

            lax.fori_loop(0, 4, self_update, 0)

            def decode(it, carry):
                last = layers - 1
                for q in range(PER - 1):
                    for half in range(2):
                        de_arrival(lax.rem(me + PER * it + 1 + q, group), half).wait_recv()

                @pl.when(it < group // PER - 1)
                def _():
                    for half in range(2):
                        de_arrival(lax.rem(me + PER * it + PER, group), half).wait_recv()

                work = []
                for q in range(PER):
                    source = lax.rem(me + PER * it + 1 + q, group)
                    for half in range(2):
                        rows = pl.ds(pl.multiple_of((half * group + source) * 256, 256), 256)
                        work.append((rows, hd[half, source], m2g[rows, :], gcur[rows, :], xst[step, :, rows]))
                def decode_task(rows, node, old, grid, state):
                    pre = dot(old, wei[last, 0:256, :]) + dot(grid, wei[last, 512:768, :])
                    term = dot(node, wei[last, 256:512, :])
                    yield
                    pre = pre + jnp.concatenate([term] * 4, axis=0)
                    y = dot(silu_of_half(pre), weo[last])
                    yield
                    edge = residual(old, norm(y))
                    pre = dot(grid, wni[last, 0:256, :]) + dot(edge, wni[last, 256:512, :])
                    yield
                    y = dot(silu_of_half(pre), wno[last])
                    yield
                    out = residual(grid, norm(y))
                    pre = dot(out, wsh[1])
                    yield
                    hidden = dot(perms[1], silu_of_half(pre))
                    yield
                    p = dot_t(wof[...], hidden.astype(BF16))
                    yield
                    new = state + stats[:, 3:4] * p + stats[:, 2:3]
                    scaled = dot_t(perms[0], ((new - mean) / std).astype(BF16))
                    yield
                    xst[step + 1, :, rows] = new
                    xs[2, rows, 0:variables] = scaled.astype(BF16)

                staggered((decode_task(*args) for args in work), 2 * PER)
                return carry

            lax.fori_loop(0, group // PER, decode, 0)
            wait_halo(1)
            for hop in range(1, group):
                for half in range(2):
                    de_copy(hop, half).wait_send()

            @pl.when(step == 0)
            def _():
                pltpu.make_async_copy(xst.at[1], out0, osem.at[0]).start()
            return carry

        lax.fori_loop(0, 2, forecast, 0)
        final = pltpu.make_async_copy(xst.at[2], out1, osem.at[1])
        final.start()
        pltpu.make_async_copy(xst.at[1], out0, osem.at[0]).wait()
        final.wait()

    def local_run(x_prev, x_cur, forcing, grid_static, g2m_feat, m2g_feat, mesh_feat, mesh_edge_feat, norm_stats, w_grid_in, w_mesh_in, w_eemb_in, w_embed_out, w_edge_in, w_edge_out, w_node_in, w_node_out, w_grid_self, w_out_hidden, w_out_final):
        grid_dev, variables = x_prev.shape
        mesh_dev = mesh_feat.shape[0]
        latent = w_embed_out.shape[-1]
        blocks = 2 * group
        perms = jnp.asarray(row_permutation(), BF16)

        vmem = pl.BlockSpec(memory_space=pltpu.VMEM)
        anywhere = pl.BlockSpec(memory_space=pl.ANY)
        state = jax.ShapeDtypeStruct((variables, grid_dev), F32)
        dma = pltpu.SemaphoreType.DMA
        first, second = pl.pallas_call(
            kernel,
            out_shape=(state, state),
            in_specs=[anywhere, anywhere] + [vmem] * 12 + [anywhere] * 4 + [vmem] * 3,
            out_specs=(anywhere, anywhere),
            scratch_shapes=[
                pltpu.VMEM(w_edge_in.shape, BF16), pltpu.VMEM(w_edge_out.shape, BF16),
                pltpu.VMEM(w_node_in.shape, BF16), pltpu.VMEM(w_node_out.shape, BF16),
                pltpu.VMEM((3, variables, grid_dev), F32), pltpu.VMEM((3, grid_dev, 128), BF16), pltpu.VMEM((grid_dev, 128), BF16),
                pltpu.VMEM((grid_dev, latent), BF16), pltpu.VMEM((grid_dev, latent), BF16), pltpu.VMEM((grid_dev, latent), BF16),
                pltpu.VMEM((grid_dev, latent), BF16),
                pltpu.VMEM((mesh_dev, latent), BF16), pltpu.VMEM((blocks, 64, 128), BF16),
                pltpu.VMEM((6, mesh_dev, latent), BF16), pltpu.VMEM((6, mesh_dev, latent), BF16),
                pltpu.VMEM((2, group, 64, latent), BF16), pltpu.VMEM((blocks, 64, latent), BF16),
                pltpu.VMEM((mesh_dev, latent), BF16), pltpu.VMEM((2, group, 64, latent), BF16),
                pltpu.VMEM((10 * blocks * 8, latent), F32), pltpu.VMEM((mesh_dev, latent), F32),
                pltpu.VMEM((2, 2, blocks, latent), BF16), pltpu.VMEM((2, 2, blocks, latent), BF16), pltpu.VMEM((4, blocks, latent), F32), pltpu.VMEM((2, latent, latent), BF16),
                pltpu.VMEM((blocks, 64, latent), BF16), pltpu.VMEM((mesh_dev, 128), BF16),
                pltpu.VMEM((2, 384, latent), BF16), pltpu.VMEM((9, 128, latent), BF16), pltpu.VMEM((2, 384, latent), F32),
                pltpu.VMEM((9, 128, latent), F32), pltpu.VMEM((-(-w_grid_in.shape[0] // 8) * 8, latent), F32),
                pltpu.VMEM((64, grid_dev), F32), pltpu.VMEM((8, mesh_dev), F32), pltpu.VMEM((48, mesh_dev), F32),
                pltpu.VMEM((8, grid_dev // 2), F32), pltpu.VMEM((8, mesh_dev // 2), F32), pltpu.VMEM((8, grid_dev // 2), F32),
                pltpu.VMEM((8, mesh_dev // 2), F32), pltpu.VMEM((2, group, 64, 128), BF16),
                dma((4,)), dma((2,)), dma((2,)), dma((2,)), dma((2,)), dma((group, 2)), dma((group, 2)), dma((group, 2)), dma((group, 2)),
                dma((group, 2)), dma((group, 2)), dma((2, 2)), dma((2, 2)),
            ],
            compiler_params=pltpu.CompilerParams(collective_id=0, has_side_effects=True, flags=FLAGS, vmem_limit_bytes=67043328),
        )(x_prev.T, x_cur.T, forcing.transpose(2, 1, 0), grid_static.T, g2m_feat.T, m2g_feat.T, mesh_feat.T, mesh_edge_feat.transpose(1, 2, 0),
          norm_stats.T, perms, w_grid_in, w_mesh_in, w_eemb_in, w_embed_out, w_edge_in, w_edge_out, w_node_in, w_node_out, w_grid_self,
          w_out_hidden, w_out_final.T)
        return first.T, second.T

    row_spec = P(("dp", "gp"))
    edge_spec = P(("dp", "gp"), None, None)
    whole = P()
    in_specs = (row_spec, row_spec, edge_spec, row_spec, row_spec, row_spec, row_spec, edge_spec, whole) + (whole,) * 11
    return jax.shard_map(local_run, mesh=mesh, in_specs=in_specs, out_specs=(row_spec, row_spec), check_vma=False)
```

```python
import jax
import jax.numpy as jnp
import numpy as np
from jax import lax
from jax.experimental import pallas as pl
from jax.experimental.pallas import tpu as pltpu
from jax.sharding import PartitionSpec as P

MESH_ID = pl.DeviceIdType.MESH
F32 = jnp.float32
BF16 = jnp.bfloat16
SUB = 256
TAIL = 256
PER = 4
WIDTH = 3
TAIL_WIDTH = 4
FLAGS = {}


def dot(a, b):
    return jnp.dot(a, b, preferred_element_type=F32)


def dot_t(a, b):
    return lax.dot_general(a, b, (((1,), (1,)), ((), ())), preferred_element_type=F32)


def silu_of_half(half):
    return (half * jnp.tanh(half) + half).astype(BF16)


def norm(y):
    z = y - jnp.mean(y, axis=-1, keepdims=True)
    return z * lax.rsqrt(jnp.mean(z * z, axis=-1, keepdims=True) + 1e-5)


def staggered(tasks, width):
    waiting = list(tasks)
    active = []
    while waiting or active:
        if waiting and len(active) < width:
            active.append(waiting.pop(0))
        for task in list(active):
            if next(task, "done") == "done":
                active.remove(task)


def together(tasks):
    active = list(tasks)
    while active:
        active = [task for task in active if next(task, "done") != "done"]


def residual(base, update):
    return (base.astype(F32) + update).astype(BF16)


def row_permutation():
    perm = np.zeros((256, 256), np.float32)
    for r in range(4):
        for j in range(8):
            for i in range(8):
                perm[r * 64 + j * 8 + i, (i * 8 + j) * 4 + r] = 1.0
    swap = np.zeros((256, 256), np.float32)
    for g in range(4):
        for j in range(8):
            for i in range(8):
                swap[g * 64 + j * 8 + i, g * 64 + i * 8 + j] = 1.0
    return np.stack([perm, perm.T, swap])


def solution(mesh):
    group = mesh.shape["gp"]

    def kernel(xp_hbm, xc_hbm, force_t, static_t, g2m_t, m2g_t, mesh_t, edge_t, stats, perms, w_grid, w_mesh, w_eemb, wembo, wei_hbm, weo_hbm, wni_hbm, wno_hbm, wgs, woh, wof,
               out0, out1,
               wei, weo, wni, wno, xst, xs, fm, g2m, m2g, glat, gcur, mlat, efl, ebase, elat, hsend, hin, hcur, hd,
               proj, recv, halo_s, halo_r, stage, wsh,
               wg, wemb, wg32, wemb32, w32, mis, msc, esc, gsnd, msnd, ghalo, mhalo, eft,
               wsem, xsem, sh_s, sh_r, osem, ef_s, ef_r, en_s, en_r, de_s, de_r, ha_s, ha_r):
        me = lax.axis_index("gp")
        left = lax.rem(me + group - 1, group)
        right = lax.rem(me + 1, group)
        blocks = 2 * group
        layers = wei_hbm.shape[0]

        barrier = pltpu.get_barrier_semaphore()
        for hop in range(1, group):
            pl.semaphore_signal(barrier, inc=1, device_id={"gp": lax.rem(me + hop, group)}, device_id_type=MESH_ID)

        weight_copies = [pltpu.make_async_copy(src, dst, wsem.at[i]) for i, (src, dst) in enumerate(
            [(wei_hbm, wei), (weo_hbm, weo), (wni_hbm, wni), (wno_hbm, wno)])]
        x_copies = [pltpu.make_async_copy(src, xst.at[i], xsem.at[i]) for i, src in enumerate((xc_hbm, xp_hbm))]
        for copy in x_copies:
            copy.start()
        for copy in weight_copies:
            copy.start()
        grid_dev = xst.shape[2]
        variables = xst.shape[1]
        half_grid = grid_dev // 2
        half_mesh = mesh_t.shape[1] // 2
        gsnd[0:g2m_t.shape[0], :] = g2m_t[:, 0:half_grid]
        msnd[0:mesh_t.shape[0], :] = mesh_t[:, 0:half_mesh]
        shift_copies = [pltpu.make_async_remote_copy(
            src_ref=src, dst_ref=dst, send_sem=sh_s.at[i], recv_sem=sh_r.at[i], device_id={"gp": left}, device_id_type=MESH_ID)
            for i, (src, dst) in enumerate(((gsnd, ghalo), (msnd, mhalo)))]

        mis[...] = jnp.zeros(mis.shape, F32)
        msc[...] = jnp.zeros(msc.shape, F32)
        esc[...] = jnp.zeros(esc.shape, F32)
        force = force_t.shape[0]
        for f in range(force):
            mis[8 * f:8 * f + 2, :] = force_t[f]
        mis[24:24 + static_t.shape[0], :] = static_t[...]
        mis[32:32 + m2g_t.shape[0], :] = m2g_t[...]
        mis[40:40 + g2m_t.shape[0], 0:half_grid] = g2m_t[:, half_grid:]
        msc[0:mesh_t.shape[0], 0:half_mesh] = mesh_t[:, half_mesh:]
        for k in range(6):
            esc[8 * k:8 * k + edge_t.shape[1], :] = edge_t[k]

        w32[0:w_grid.shape[0], :] = w_grid[...].astype(F32) * 0.5
        wg32[...] = jnp.zeros(wg32.shape, F32)
        wemb32[...] = jnp.zeros(wemb32.shape, F32)
        for s in range(2):
            wg32[s, 0:variables, :] = w32[0:variables, :]
            wg32[s, 128:128 + variables, :] = w32[variables:2 * variables, :]
            for f in range(force):
                wg32[s, 256 + 8 * f + s:257 + 8 * f + s, :] = w32[2 * variables + f:2 * variables + f + 1, :]
            for f in range(static_t.shape[0]):
                at = 2 * variables + force + f
                wg32[s, 280 + f:281 + f, :] = w32[at:at + 1, :]
            wg[s] = wg32[s].astype(BF16)
        places = [(40, w_eemb[0]), (32, w_eemb[1]), (0, w_mesh[...])] + [(8 * k, w_eemb[2]) for k in range(6)]
        for i, (at, rows) in enumerate(places):
            wemb32[i, at:at + rows.shape[0], :] = rows.astype(F32) * 0.5
            wemb[i] = wemb32[i].astype(BF16)

        def wide(rows):
            return jnp.concatenate([rows, jnp.zeros((128 - rows.shape[0], rows.shape[1]), F32)], axis=0).astype(BF16)

        for q in range(4):
            feats = dot_t(perms[2], wide(esc[:, q * 256:q * 256 + 256])).astype(BF16)
            for g in range(4):
                chunk = 4 * q + g
                eft[chunk // group, chunk % group] = feats[g * 64:g * 64 + 64]
        for slot in range(3):
            xs[slot] = jnp.zeros(xs.shape[1:], BF16)
        pl.semaphore_wait(barrier, group - 1)
        for copy in shift_copies:
            copy.start()

        def block_of(device, half):
            return lax.rem(2 * device + half, blocks)

        def ef_copy(hop, half):
            dest = lax.rem(me + hop, group)
            return pltpu.make_async_remote_copy(
                src_ref=eft.at[half, dest], dst_ref=efl.at[2 * me + half], send_sem=ef_s.at[dest, half],
                recv_sem=ef_r.at[me, half], device_id={"gp": dest}, device_id_type=MESH_ID)

        def ef_keep(half):
            return pltpu.make_async_copy(eft.at[half, me], efl.at[2 * me + half], ef_r.at[me, half])

        for half in range(2):
            for hop in range(1, group):
                ef_copy(hop, half).start()
            ef_keep(half).start()

        for copy in x_copies:
            copy.wait()
        mean = stats[:, 0:1]
        std = stats[:, 1:2]

        def embed_task(rows):
            misc = dot_t(perms[0], wide(mis[:, rows]))
            prev = dot_t(perms[0], ((xst[1, :, rows] - mean) / std).astype(BF16))
            cur = dot_t(perms[0], ((xst[0, :, rows] - mean) / std).astype(BF16))
            yield
            misc = misc.astype(BF16)
            fm[rows, :] = misc
            xs[0, rows, 0:variables] = prev.astype(BF16)
            xs[1, rows, 0:variables] = cur.astype(BF16)
            first = dot(misc, wemb[0])
            second = dot(misc, wemb[1])
            yield
            first = dot(silu_of_half(first), wembo[2])
            second = dot(silu_of_half(second), wembo[3])
            yield
            g2m[rows, :] = norm(first).astype(BF16)
            m2g[rows, :] = norm(second).astype(BF16)

        def embed_rows(it, carry):
            together(embed_task(pl.ds(pl.multiple_of((it * 4 + sub) * 256, 256), 256)) for sub in range(4))
            return carry

        lax.fori_loop(0, 2, embed_rows, 0)
        for copy in shift_copies:
            copy.wait_recv()
        mis[40:40 + g2m_t.shape[0], half_grid:] = ghalo[0:g2m_t.shape[0], :]
        msc[0:mesh_t.shape[0], half_mesh:] = mhalo[0:mesh_t.shape[0], :]
        lax.fori_loop(2, 4, embed_rows, 0)
        for copy in shift_copies:
            copy.wait_send()

        def plain_task(get, put, w_first, w_second):
            y = dot(get(), w_first)
            yield
            y = dot(silu_of_half(y), w_second)
            yield
            put(norm(y))

        def mesh_task(rows):
            def put(y):
                mlat[rows, :] = y.astype(BF16)
            feats = dot_t(perms[2], wide(msc[:, rows])).astype(BF16)
            return plain_task(lambda: feats, put, wemb[2], wembo[1])

        together(mesh_task(slice(sub * 256, sub * 256 + 256)) for sub in range(4))
        for copy in weight_copies:
            copy.wait()

        def halve(layer, carry):
            wei[layer] = wei[layer] * 0.5
            wni[layer] = wni[layer] * 0.5
            return carry

        lax.fori_loop(0, layers, halve, 0)
        wsh[0] = wgs[0] * 0.5
        wsh[1] = woh[...] * 0.5

        def en_copy(hop, half):
            dest = lax.rem(me + hop, group)
            return pltpu.make_async_remote_copy(
                src_ref=hsend.at[half, dest], dst_ref=hin.at[block_of(me, 1 + half)], send_sem=en_s.at[dest, half],
                recv_sem=en_r.at[me, half], device_id={"gp": dest}, device_id_type=MESH_ID)

        def de_copy(hop, half):
            dest = lax.rem(me + hop, group)
            return pltpu.make_async_remote_copy(
                src_ref=hcur.at[block_of(dest, 1 + half)], dst_ref=hd.at[half, me], send_sem=de_s.at[dest, half],
                recv_sem=de_r.at[me, half], device_id={"gp": dest}, device_id_type=MESH_ID)

        def en_arrival(source, half):
            return pltpu.make_async_remote_copy(
                src_ref=hsend.at[half, me], dst_ref=hin.at[block_of(source, 1 + half)], send_sem=en_s.at[me, half],
                recv_sem=en_r.at[source, half], device_id={"gp": left}, device_id_type=MESH_ID)

        def de_arrival(source, half):
            return pltpu.make_async_remote_copy(
                src_ref=hcur.at[0], dst_ref=hd.at[half, source], send_sem=de_s.at[me, half],
                recv_sem=de_r.at[source, half], device_id={"gp": left}, device_id_type=MESH_ID)

        def ef_arrival(source, half):
            return pltpu.make_async_remote_copy(
                src_ref=eft.at[half, me], dst_ref=efl.at[2 * source + half], send_sem=ef_s.at[me, half],
                recv_sem=ef_r.at[source, half], device_id={"gp": left}, device_id_type=MESH_ID)

        def halo_copies(slot):
            return [pltpu.make_async_remote_copy(
                src_ref=halo_s.at[slot, side], dst_ref=halo_r.at[slot, 1 - side], send_sem=ha_s.at[slot, side],
                recv_sem=ha_r.at[slot, 1 - side], device_id={"gp": (left, right)[side]}, device_id_type=MESH_ID)
                for side in range(2)]

        def send_halo(slot):
            for b in range(blocks):
                stage[0, b:b + 1, :] = hcur[b, 0:16, :].astype(F32)[0:1]
                stage[1, b:b + 1, :] = hcur[b, 48:64, :].astype(F32)[15:16]
            halo_s[slot, 0] = stage[0].astype(BF16)
            halo_s[slot, 1] = stage[1].astype(BF16)
            for copy in halo_copies(slot):
                copy.start()

        def edge_task(layer, k, sub, size, send):
            rows = slice(sub, sub + size)
            old = elat[k, rows, :]
            pre = dot(old, wei[layer, 0:256, :]) + (send + recv[rows, :])
            yield
            y = dot(silu_of_half(pre), weo[layer])
            yield
            elat[k, rows, :] = residual(old, norm(y))

        def project(layer, lo, hi):
            h = hcur[lo:hi].reshape((hi - lo) * 64, 256)
            return dot(h, wei[layer, 256:512, :]), dot(h, wei[layer, 512:768, :])

        def put_projections(lo, hi, send, receive):
            proj[lo:hi, 8:72, :] = send.reshape(hi - lo, 64, 256)
            recv[lo * 64:hi * 64, :] = receive

        def tail_task(layer, lo, hi):
            size = (hi - lo) * 64
            rows = slice(lo * 64, hi * 64)
            olds = [elat[k, rows, :] for k in range(2)]
            sends = [proj[lo:hi, 16:80, :].reshape(size, 256), proj[lo:hi, 0:64, :].reshape(size, 256)]
            pres = [dot(old, wei[layer, 0:256, :]) + (send + recv[rows, :]) for old, send in zip(olds, sends)]
            total = elat[2, rows, :].astype(F32)
            for k in range(3, 6):
                total = total + elat[k, rows, :].astype(F32)
            yield
            ys = [dot(silu_of_half(pre), weo[layer]) for pre in pres]
            yield
            for k in range(2):
                new = residual(olds[k], norm(ys[k]))
                elat[k, rows, :] = new
                total = total + new.astype(F32)
            node = hcur[lo:hi].reshape(size, 256)
            pre = dot(node, wni[layer, 0:256, :]) + dot(total.astype(BF16), wni[layer, 256:512, :])
            yield
            y = dot(silu_of_half(pre), wno[layer])
            yield
            new = residual(node, norm(y))
            hcur[lo:hi] = new.reshape(hi - lo, 64, 256)
            send = dot(new, wei[layer + 1, 256:512, :])
            receive = dot(new, wei[layer + 1, 512:768, :])
            yield
            put_projections(lo, hi, send, receive)

        def rolled(shift, sub, size):
            lo, count = sub // 64, size // 64
            picks = [(lo + q + shift) % blocks for q in range(count)]
            return jnp.concatenate([proj[b, 8:72, :] for b in picks], axis=0)

        def mesh_layer(layer, carry):
            slot = lax.rem(layer, 2)
            staggered((edge_task(layer, k, sub, SUB, rolled(shift, sub, SUB))
                       for k, shift in ((2, 1), (3, -1), (4, 4), (5, -4)) for sub in range(0, blocks * 64, SUB)), WIDTH)
            for copy in halo_copies(slot):
                copy.wait_recv()
            for copy in halo_copies(slot):
                copy.wait_send()
            edge_proj = dot(halo_r[slot].reshape(32, 256), wei[layer, 256:512, :])
            low = edge_proj[0:16]
            high = edge_proj[16:32]
            stage[0] = jnp.where(me == 0, jnp.concatenate([low[15:16], low[0:15]], axis=0), low)
            stage[1] = jnp.where(me == group - 1, jnp.concatenate([high[1:16], high[0:1]], axis=0), high)
            sublane = lax.broadcasted_iota(jnp.int32, (8, 256), 0)
            for b in range(blocks):
                proj[b, 0:8, :] = jnp.where(sublane == 0, stage[0, b:b + 1, :], pltpu.roll(proj[b, 64:72, :], 1, 0))
                proj[b, 72:80, :] = jnp.where(sublane == 7, stage[1, b:b + 1, :], pltpu.roll(proj[b, 8:16, :], 7, 0))
            staggered((tail_task(layer, lo, lo + TAIL // 64) for lo in range(0, blocks, TAIL // 64)), TAIL_WIDTH)

            @pl.when(layer < layers - 2)
            def _():
                send_halo(1 - slot)
            return carry

        def forecast(step, carry):
            def encode_task(dest, half):
                chunk = half * group + dest
                rows = pl.ds(pl.multiple_of(chunk * 256, 256), 256)
                feats = jnp.concatenate([xs[step, rows, :], xs[step + 1, rows, :]], axis=1)
                node = mlat[pl.ds(pl.multiple_of(chunk * 64, 64), 64), :]
                old = g2m[rows, :]
                pre = dot(feats, wg[step, 0:256, :]) + dot(fm[rows, :], wg[step, 256:384, :])
                yield
                y = dot(silu_of_half(pre), wembo[0])
                yield
                lat = norm(y).astype(BF16)
                glat[rows, :] = lat
                pre = dot(old, wei[0, 0:256, :]) + dot(lat, wei[0, 256:512, :])
                term = dot(node, wei[0, 512:768, :])
                yield
                pre = pre + jnp.concatenate([term] * 4, axis=0)
                y = dot(silu_of_half(pre), weo[0])
                yield
                edge = residual(old, norm(y)).astype(F32)
                return node, (edge[0:64] + edge[64:128] + edge[128:192] + edge[192:256]).astype(BF16)

            def encode_group(pairs):
                results = []

                def run(dest, half):
                    results.append((yield from encode_task(dest, half)))

                active = [run(dest, half) for dest, half in pairs]
                while active:
                    active = [task for task in active if next(task, "done") != "done"]
                    yield
                node = jnp.concatenate([r[0] for r in results], axis=0)
                esum = jnp.concatenate([r[1] for r in results], axis=0)
                pre = dot(node, wni[0, 0:256, :]) + dot(esum, wni[0, 256:512, :])
                yield
                y = dot(silu_of_half(pre), wno[0])
                yield
                new = residual(node, norm(y))
                for q, (dest, half) in enumerate(pairs):
                    hsend[half, dest] = new[q * 64:q * 64 + 64]

            def encode(it, carry):
                dests = [lax.rem(me + PER * it + 1 + q, group) for q in range(PER)]
                pairs = [(dest, half) for dest in dests for half in range(2)]
                staggered((encode_group(pairs[lo:lo + 4]) for lo in range(0, 2 * PER, 4)), 4)
                for q in range(PER - 1):
                    for half in range(2):
                        en_copy(PER * it + 1 + q, half).start()

                @pl.when(it < group // PER - 1)
                def _():
                    for half in range(2):
                        en_copy(PER * it + PER, half).start()
                return carry

            lax.fori_loop(0, group // PER, encode, 0)

            @pl.when(step == 0)
            def _():
                for half in range(2):
                    for hop in range(1, group):
                        ef_arrival(lax.rem(me + hop, group), half).wait_recv()
                    ef_keep(half).wait()

                def embed_edges(k, carry):
                    def edge_embed_task(sub):
                        def put(y):
                            ebase[k, sub * 64:sub * 64 + 256, :] = y.astype(BF16)
                        return plain_task(lambda: efl[sub:sub + 4].reshape(256, 128), put, wemb[3 + k], wembo[4])

                    together(edge_embed_task(sub) for sub in range(0, blocks, 4))
                    return carry

                lax.fori_loop(0, 6, embed_edges, 0)
                for hop in range(1, group):
                    for half in range(2):
                        ef_copy(hop, half).wait_send()

            elat[...] = ebase[...]
            for hop in range(1, group):
                for half in range(2):
                    en_arrival(lax.rem(me + hop, group), half).wait_recv()
            for hop in range(1, group):
                for half in range(2):
                    en_copy(hop, half).wait_send()
            hcur[...] = hin[...]
            for half in range(2):
                hcur[block_of(me, 1 + half)] = hsend[half, me]
            send_halo(1)
            put_projections(0, blocks, *project(1, 0, blocks))
            lax.fori_loop(1, layers - 1, mesh_layer, 0)
            for hop in range(1, group):
                for half in range(2):
                    de_copy(hop, half).start()
            for half in range(2):
                hd[half, me] = hcur[block_of(me, 1 + half)]

            def self_task(rows):
                old = glat[rows, :]

                def put(y):
                    gcur[rows, :] = residual(old, y)
                return plain_task(lambda: old, put, wsh[0], wgs[1])

            def self_update(it, carry):
                together(self_task(pl.ds(pl.multiple_of((it * 4 + sub) * 256, 256), 256)) for sub in range(4))
                return carry

            lax.fori_loop(0, 4, self_update, 0)

            def decode(it, carry):
                last = layers - 1
                for q in range(PER - 1):
                    for half in range(2):
                        de_arrival(lax.rem(me + 2 * group - PER * it - 1 - q, group), half).wait_recv()

                @pl.when(it < group // PER - 1)
                def _():
                    for half in range(2):
                        de_arrival(lax.rem(me + 2 * group - PER * it - PER, group), half).wait_recv()

                work = []
                for q in range(PER):
                    source = lax.rem(me + 2 * group - PER * it - 1 - q, group)
                    for half in range(2):
                        rows = pl.ds(pl.multiple_of((half * group + source) * 256, 256), 256)
                        work.append((rows, hd[half, source], m2g[rows, :], gcur[rows, :], xst[step, :, rows]))
                def decode_task(rows, node, old, grid, state):
                    pre = dot(old, wei[last, 0:256, :]) + dot(grid, wei[last, 512:768, :])
                    term = dot(node, wei[last, 256:512, :])
                    yield
                    pre = pre + jnp.concatenate([term] * 4, axis=0)
                    y = dot(silu_of_half(pre), weo[last])
                    yield
                    edge = residual(old, norm(y))
                    pre = dot(grid, wni[last, 0:256, :]) + dot(edge, wni[last, 256:512, :])
                    yield
                    y = dot(silu_of_half(pre), wno[last])
                    yield
                    out = residual(grid, norm(y))
                    pre = dot(out, wsh[1])
                    yield
                    hidden = dot(perms[1], silu_of_half(pre))
                    yield
                    p = dot_t(wof[...], hidden.astype(BF16))
                    yield
                    new = state + stats[:, 3:4] * p + stats[:, 2:3]
                    scaled = dot_t(perms[0], ((new - mean) / std).astype(BF16))
                    yield
                    xst[step + 1, :, rows] = new
                    xs[2, rows, 0:variables] = scaled.astype(BF16)

                staggered((decode_task(*args) for args in work), 2 * PER)
                return carry

            lax.fori_loop(0, group // PER, decode, 0)
            for hop in range(1, group):
                for half in range(2):
                    de_copy(hop, half).wait_send()

            @pl.when(step == 0)
            def _():
                pltpu.make_async_copy(xst.at[1], out0, osem.at[0]).start()
            return carry

        lax.fori_loop(0, 2, forecast, 0)
        final = pltpu.make_async_copy(xst.at[2], out1, osem.at[1])
        final.start()
        pltpu.make_async_copy(xst.at[1], out0, osem.at[0]).wait()
        final.wait()

    def local_run(x_prev, x_cur, forcing, grid_static, g2m_feat, m2g_feat, mesh_feat, mesh_edge_feat, norm_stats, w_grid_in, w_mesh_in, w_eemb_in, w_embed_out, w_edge_in, w_edge_out, w_node_in, w_node_out, w_grid_self, w_out_hidden, w_out_final):
        grid_dev, variables = x_prev.shape
        mesh_dev = mesh_feat.shape[0]
        latent = w_embed_out.shape[-1]
        blocks = 2 * group
        perms = jnp.asarray(row_permutation(), BF16)

        vmem = pl.BlockSpec(memory_space=pltpu.VMEM)
        anywhere = pl.BlockSpec(memory_space=pl.ANY)
        state = jax.ShapeDtypeStruct((variables, grid_dev), F32)
        dma = pltpu.SemaphoreType.DMA
        first, second = pl.pallas_call(
            kernel,
            out_shape=(state, state),
            in_specs=[anywhere, anywhere] + [vmem] * 12 + [anywhere] * 4 + [vmem] * 3,
            out_specs=(anywhere, anywhere),
            scratch_shapes=[
                pltpu.VMEM(w_edge_in.shape, BF16), pltpu.VMEM(w_edge_out.shape, BF16),
                pltpu.VMEM(w_node_in.shape, BF16), pltpu.VMEM(w_node_out.shape, BF16),
                pltpu.VMEM((3, variables, grid_dev), F32), pltpu.VMEM((3, grid_dev, 128), BF16), pltpu.VMEM((grid_dev, 128), BF16),
                pltpu.VMEM((grid_dev, latent), BF16), pltpu.VMEM((grid_dev, latent), BF16), pltpu.VMEM((grid_dev, latent), BF16),
                pltpu.VMEM((grid_dev, latent), BF16),
                pltpu.VMEM((mesh_dev, latent), BF16), pltpu.VMEM((blocks, 64, 128), BF16),
                pltpu.VMEM((6, mesh_dev, latent), BF16), pltpu.VMEM((6, mesh_dev, latent), BF16),
                pltpu.VMEM((2, group, 64, latent), BF16), pltpu.VMEM((blocks, 64, latent), BF16),
                pltpu.VMEM((blocks, 64, latent), BF16), pltpu.VMEM((2, group, 64, latent), BF16),
                pltpu.VMEM((blocks, 80, latent), F32), pltpu.VMEM((mesh_dev, latent), F32),
                pltpu.VMEM((2, 2, blocks, latent), BF16), pltpu.VMEM((2, 2, blocks, latent), BF16), pltpu.VMEM((2, blocks, latent), F32), pltpu.VMEM((2, latent, latent), BF16),
                pltpu.VMEM((2, 384, latent), BF16), pltpu.VMEM((9, 128, latent), BF16), pltpu.VMEM((2, 384, latent), F32),
                pltpu.VMEM((9, 128, latent), F32), pltpu.VMEM((-(-w_grid_in.shape[0] // 8) * 8, latent), F32),
                pltpu.VMEM((64, grid_dev), F32), pltpu.VMEM((8, mesh_dev), F32), pltpu.VMEM((48, mesh_dev), F32),
                pltpu.VMEM((8, grid_dev // 2), F32), pltpu.VMEM((8, mesh_dev // 2), F32), pltpu.VMEM((8, grid_dev // 2), F32),
                pltpu.VMEM((8, mesh_dev // 2), F32), pltpu.VMEM((2, group, 64, 128), BF16),
                dma((4,)), dma((2,)), dma((2,)), dma((2,)), dma((2,)), dma((group, 2)), dma((group, 2)), dma((group, 2)), dma((group, 2)),
                dma((group, 2)), dma((group, 2)), dma((2, 2)), dma((2, 2)),
            ],
            compiler_params=pltpu.CompilerParams(collective_id=0, has_side_effects=True, flags=FLAGS, vmem_limit_bytes=67043328),
        )(x_prev.T, x_cur.T, forcing.transpose(2, 1, 0), grid_static.T, g2m_feat.T, m2g_feat.T, mesh_feat.T, mesh_edge_feat.transpose(1, 2, 0),
          norm_stats.T, perms, w_grid_in, w_mesh_in, w_eemb_in, w_embed_out, w_edge_in, w_edge_out, w_node_in, w_node_out, w_grid_self,
          w_out_hidden, w_out_final.T)
        return first.T, second.T

    row_spec = P(("dp", "gp"))
    edge_spec = P(("dp", "gp"), None, None)
    whole = P()
    in_specs = (row_spec, row_spec, edge_spec, row_spec, row_spec, row_spec, row_spec, edge_spec, whole) + (whole,) * 11
    return jax.shard_map(local_run, mesh=mesh, in_specs=in_specs, out_specs=(row_spec, row_spec), check_vma=False)
```

```python
import jax
import jax.numpy as jnp
import numpy as np
from jax import lax
from jax.experimental import pallas as pl
from jax.experimental.pallas import tpu as pltpu
from jax.sharding import PartitionSpec as P

MESH_ID = pl.DeviceIdType.MESH
F32 = jnp.float32
BF16 = jnp.bfloat16
SUB = 256
TAIL = 512
PER = 4
WIDTH = 3
TAIL_WIDTH = 4
FLAGS = {}


def dot(a, b):
    return jnp.dot(a, b, preferred_element_type=F32)


def dot_t(a, b):
    return lax.dot_general(a, b, (((1,), (1,)), ((), ())), preferred_element_type=F32)


def silu_of_half(half):
    return (half * jnp.tanh(half) + half).astype(BF16)


def norm(y):
    z = y - jnp.mean(y, axis=-1, keepdims=True)
    return z * lax.rsqrt(jnp.mean(z * z, axis=-1, keepdims=True) + 1e-5)


def staggered(tasks, width):
    waiting = list(tasks)
    active = []
    while waiting or active:
        if waiting and len(active) < width:
            active.append(waiting.pop(0))
        for task in list(active):
            if next(task, "done") == "done":
                active.remove(task)


def together(tasks):
    active = list(tasks)
    while active:
        active = [task for task in active if next(task, "done") != "done"]


def residual(base, update):
    return (base.astype(F32) + update).astype(BF16)


def row_permutation():
    perm = np.zeros((256, 256), np.float32)
    for r in range(4):
        for j in range(8):
            for i in range(8):
                perm[r * 64 + j * 8 + i, (i * 8 + j) * 4 + r] = 1.0
    swap = np.zeros((256, 256), np.float32)
    for g in range(4):
        for j in range(8):
            for i in range(8):
                swap[g * 64 + j * 8 + i, g * 64 + i * 8 + j] = 1.0
    return np.stack([perm, perm.T, swap])


def solution(mesh):
    group = mesh.shape["gp"]

    def kernel(xp_hbm, xc_hbm, force_t, static_t, g2m_t, m2g_t, mesh_t, edge_t, stats, perms, w_grid, w_mesh, w_eemb, wembo, wei_hbm, weo_hbm, wni_hbm, wno_hbm, wgs, woh, wof,
               out0, out1,
               wei, weo, wni, wno, xst, xs, fm, g2m, m2g, glat, gcur, mlat, efl, ebase, elat, hsend, hin, hcur, hd,
               proj, recv, halo_s, halo_r, stage, wsh,
               wg, wemb, wg32, wemb32, w32, mis, msc, esc, gsnd, msnd, ghalo, mhalo, eft,
               wsem, xsem, sh_s, sh_r, osem, ef_s, ef_r, en_s, en_r, de_s, de_r, ha_s, ha_r):
        me = lax.axis_index("gp")
        left = lax.rem(me + group - 1, group)
        right = lax.rem(me + 1, group)
        blocks = 2 * group
        layers = wei_hbm.shape[0]

        barrier = pltpu.get_barrier_semaphore()
        for hop in range(1, group):
            pl.semaphore_signal(barrier, inc=1, device_id={"gp": lax.rem(me + hop, group)}, device_id_type=MESH_ID)

        weight_copies = [pltpu.make_async_copy(src, dst, wsem.at[i]) for i, (src, dst) in enumerate(
            [(wei_hbm, wei), (weo_hbm, weo), (wni_hbm, wni), (wno_hbm, wno)])]
        x_copies = [pltpu.make_async_copy(src, xst.at[i], xsem.at[i]) for i, src in enumerate((xc_hbm, xp_hbm))]
        for copy in x_copies:
            copy.start()
        for copy in weight_copies:
            copy.start()
        grid_dev = xst.shape[2]
        variables = xst.shape[1]
        half_grid = grid_dev // 2
        half_mesh = mesh_t.shape[1] // 2
        gsnd[0:g2m_t.shape[0], :] = g2m_t[:, 0:half_grid]
        msnd[0:mesh_t.shape[0], :] = mesh_t[:, 0:half_mesh]
        shift_copies = [pltpu.make_async_remote_copy(
            src_ref=src, dst_ref=dst, send_sem=sh_s.at[i], recv_sem=sh_r.at[i], device_id={"gp": left}, device_id_type=MESH_ID)
            for i, (src, dst) in enumerate(((gsnd, ghalo), (msnd, mhalo)))]

        mis[...] = jnp.zeros(mis.shape, F32)
        msc[...] = jnp.zeros(msc.shape, F32)
        esc[...] = jnp.zeros(esc.shape, F32)
        force = force_t.shape[0]
        for f in range(force):
            mis[8 * f:8 * f + 2, :] = force_t[f]
        mis[24:24 + static_t.shape[0], :] = static_t[...]
        mis[32:32 + m2g_t.shape[0], :] = m2g_t[...]
        mis[40:40 + g2m_t.shape[0], 0:half_grid] = g2m_t[:, half_grid:]
        msc[0:mesh_t.shape[0], 0:half_mesh] = mesh_t[:, half_mesh:]
        for k in range(6):
            esc[8 * k:8 * k + edge_t.shape[1], :] = edge_t[k]

        w32[0:w_grid.shape[0], :] = w_grid[...].astype(F32) * 0.5
        wg32[...] = jnp.zeros(wg32.shape, F32)
        wemb32[...] = jnp.zeros(wemb32.shape, F32)
        for s in range(2):
            wg32[s, 0:variables, :] = w32[0:variables, :]
            wg32[s, 128:128 + variables, :] = w32[variables:2 * variables, :]
            for f in range(force):
                wg32[s, 256 + 8 * f + s:257 + 8 * f + s, :] = w32[2 * variables + f:2 * variables + f + 1, :]
            for f in range(static_t.shape[0]):
                at = 2 * variables + force + f
                wg32[s, 280 + f:281 + f, :] = w32[at:at + 1, :]
            wg[s] = wg32[s].astype(BF16)
        places = [(40, w_eemb[0]), (32, w_eemb[1]), (0, w_mesh[...])] + [(8 * k, w_eemb[2]) for k in range(6)]
        for i, (at, rows) in enumerate(places):
            wemb32[i, at:at + rows.shape[0], :] = rows.astype(F32) * 0.5
            wemb[i] = wemb32[i].astype(BF16)

        def wide(rows):
            return jnp.concatenate([rows, jnp.zeros((128 - rows.shape[0], rows.shape[1]), F32)], axis=0).astype(BF16)

        for q in range(4):
            feats = dot_t(perms[2], wide(esc[:, q * 256:q * 256 + 256])).astype(BF16)
            for g in range(4):
                chunk = 4 * q + g
                eft[chunk // group, chunk % group] = feats[g * 64:g * 64 + 64]
        for slot in range(3):
            xs[slot] = jnp.zeros(xs.shape[1:], BF16)
        pl.semaphore_wait(barrier, group - 1)
        for copy in shift_copies:
            copy.start()

        def block_of(device, half):
            return lax.rem(2 * device + half, blocks)

        def ef_copy(hop, half):
            dest = lax.rem(me + hop, group)
            return pltpu.make_async_remote_copy(
                src_ref=eft.at[half, dest], dst_ref=efl.at[2 * me + half], send_sem=ef_s.at[dest, half],
                recv_sem=ef_r.at[me, half], device_id={"gp": dest}, device_id_type=MESH_ID)

        def ef_keep(half):
            return pltpu.make_async_copy(eft.at[half, me], efl.at[2 * me + half], ef_r.at[me, half])

        for half in range(2):
            for hop in range(1, group):
                ef_copy(hop, half).start()
            ef_keep(half).start()

        for copy in x_copies:
            copy.wait()
        mean = stats[:, 0:1]
        std = stats[:, 1:2]

        def embed_task(rows):
            misc = dot_t(perms[0], wide(mis[:, rows]))
            prev = dot_t(perms[0], ((xst[1, :, rows] - mean) / std).astype(BF16))
            cur = dot_t(perms[0], ((xst[0, :, rows] - mean) / std).astype(BF16))
            yield
            misc = misc.astype(BF16)
            fm[rows, :] = misc
            xs[0, rows, 0:variables] = prev.astype(BF16)
            xs[1, rows, 0:variables] = cur.astype(BF16)
            first = dot(misc, wemb[0])
            second = dot(misc, wemb[1])
            yield
            first = dot(silu_of_half(first), wembo[2])
            second = dot(silu_of_half(second), wembo[3])
            yield
            g2m[rows, :] = norm(first).astype(BF16)
            m2g[rows, :] = norm(second).astype(BF16)

        def embed_rows(it, carry):
            together(embed_task(pl.ds(pl.multiple_of((it * 4 + sub) * 256, 256), 256)) for sub in range(4))
            return carry

        lax.fori_loop(0, 2, embed_rows, 0)
        for copy in shift_copies:
            copy.wait_recv()
        mis[40:40 + g2m_t.shape[0], half_grid:] = ghalo[0:g2m_t.shape[0], :]
        msc[0:mesh_t.shape[0], half_mesh:] = mhalo[0:mesh_t.shape[0], :]
        lax.fori_loop(2, 4, embed_rows, 0)
        for copy in shift_copies:
            copy.wait_send()

        def plain_task(get, put, w_first, w_second):
            y = dot(get(), w_first)
            yield
            y = dot(silu_of_half(y), w_second)
            yield
            put(norm(y))

        def mesh_task(rows):
            def put(y):
                mlat[rows, :] = y.astype(BF16)
            feats = dot_t(perms[2], wide(msc[:, rows])).astype(BF16)
            return plain_task(lambda: feats, put, wemb[2], wembo[1])

        together(mesh_task(slice(sub * 256, sub * 256 + 256)) for sub in range(4))
        for copy in weight_copies:
            copy.wait()

        def halve(layer, carry):
            wei[layer] = wei[layer] * 0.5
            wni[layer] = wni[layer] * 0.5
            return carry

        lax.fori_loop(0, layers, halve, 0)
        wsh[0] = wgs[0] * 0.5
        wsh[1] = woh[...] * 0.5

        def en_copy(hop, half):
            dest = lax.rem(me + hop, group)
            return pltpu.make_async_remote_copy(
                src_ref=hsend.at[half, dest], dst_ref=hin.at[block_of(me, 1 + half)], send_sem=en_s.at[dest, half],
                recv_sem=en_r.at[me, half], device_id={"gp": dest}, device_id_type=MESH_ID)

        def de_copy(hop, half):
            dest = lax.rem(me + hop, group)
            return pltpu.make_async_remote_copy(
                src_ref=hcur.at[block_of(dest, 1 + half)], dst_ref=hd.at[half, me], send_sem=de_s.at[dest, half],
                recv_sem=de_r.at[me, half], device_id={"gp": dest}, device_id_type=MESH_ID)

        def en_arrival(source, half):
            return pltpu.make_async_remote_copy(
                src_ref=hsend.at[half, me], dst_ref=hin.at[block_of(source, 1 + half)], send_sem=en_s.at[me, half],
                recv_sem=en_r.at[source, half], device_id={"gp": left}, device_id_type=MESH_ID)

        def de_arrival(source, half):
            return pltpu.make_async_remote_copy(
                src_ref=hcur.at[0], dst_ref=hd.at[half, source], send_sem=de_s.at[me, half],
                recv_sem=de_r.at[source, half], device_id={"gp": left}, device_id_type=MESH_ID)

        def ef_arrival(source, half):
            return pltpu.make_async_remote_copy(
                src_ref=eft.at[half, me], dst_ref=efl.at[2 * source + half], send_sem=ef_s.at[me, half],
                recv_sem=ef_r.at[source, half], device_id={"gp": left}, device_id_type=MESH_ID)

        def halo_copies(slot):
            return [pltpu.make_async_remote_copy(
                src_ref=halo_s.at[slot, side], dst_ref=halo_r.at[slot, 1 - side], send_sem=ha_s.at[slot, side],
                recv_sem=ha_r.at[slot, 1 - side], device_id={"gp": (left, right)[side]}, device_id_type=MESH_ID)
                for side in range(2)]

        def send_halo(slot):
            for b in range(blocks):
                stage[0, b:b + 1, :] = hcur[b, 0:16, :].astype(F32)[0:1]
                stage[1, b:b + 1, :] = hcur[b, 48:64, :].astype(F32)[15:16]
            halo_s[slot, 0] = stage[0].astype(BF16)
            halo_s[slot, 1] = stage[1].astype(BF16)
            for copy in halo_copies(slot):
                copy.start()

        def edge_task(layer, k, sub, size, send):
            rows = slice(sub, sub + size)
            old = elat[k, rows, :]
            pre = dot(old, wei[layer, 0:256, :]) + (send + recv[rows, :])
            yield
            y = dot(silu_of_half(pre), weo[layer])
            yield
            elat[k, rows, :] = residual(old, norm(y))

        def project(layer, lo, hi):
            h = hcur[lo:hi].reshape((hi - lo) * 64, 256)
            return dot(h, wei[layer, 256:512, :]), dot(h, wei[layer, 512:768, :])

        def put_projections(lo, hi, send, receive):
            proj[lo:hi, 8:72, :] = send.reshape(hi - lo, 64, 256)
            recv[lo * 64:hi * 64, :] = receive

        def tail_task(layer, lo, hi):
            size = (hi - lo) * 64
            rows = slice(lo * 64, hi * 64)
            olds = [elat[k, rows, :] for k in range(2)]
            sends = [proj[lo:hi, 16:80, :].reshape(size, 256), proj[lo:hi, 0:64, :].reshape(size, 256)]
            pres = [dot(old, wei[layer, 0:256, :]) + (send + recv[rows, :]) for old, send in zip(olds, sends)]
            total = elat[2, rows, :].astype(F32)
            for k in range(3, 6):
                total = total + elat[k, rows, :].astype(F32)
            yield
            ys = [dot(silu_of_half(pre), weo[layer]) for pre in pres]
            yield
            for k in range(2):
                new = residual(olds[k], norm(ys[k]))
                elat[k, rows, :] = new
                total = total + new.astype(F32)
            node = hcur[lo:hi].reshape(size, 256)
            pre = dot(node, wni[layer, 0:256, :]) + dot(total.astype(BF16), wni[layer, 256:512, :])
            yield
            y = dot(silu_of_half(pre), wno[layer])
            yield
            new = residual(node, norm(y))
            hcur[lo:hi] = new.reshape(hi - lo, 64, 256)
            send = dot(new, wei[layer + 1, 256:512, :])
            receive = dot(new, wei[layer + 1, 512:768, :])
            yield
            put_projections(lo, hi, send, receive)

        def rolled(shift, sub, size):
            lo, count = sub // 64, size // 64
            picks = [(lo + q + shift) % blocks for q in range(count)]
            return jnp.concatenate([proj[b, 8:72, :] for b in picks], axis=0)

        def mesh_layer(layer, carry):
            slot = lax.rem(layer, 2)
            staggered((edge_task(layer, k, sub, SUB, rolled(shift, sub, SUB))
                       for k, shift in ((2, 1), (3, -1), (4, 4), (5, -4)) for sub in range(0, blocks * 64, SUB)), WIDTH)
            for copy in halo_copies(slot):
                copy.wait_recv()
            for copy in halo_copies(slot):
                copy.wait_send()
            edge_proj = dot(halo_r[slot].reshape(32, 256), wei[layer, 256:512, :])
            low = edge_proj[0:16]
            high = edge_proj[16:32]
            stage[0] = jnp.where(me == 0, jnp.concatenate([low[15:16], low[0:15]], axis=0), low)
            stage[1] = jnp.where(me == group - 1, jnp.concatenate([high[1:16], high[0:1]], axis=0), high)
            sublane = lax.broadcasted_iota(jnp.int32, (8, 256), 0)
            for b in range(blocks):
                proj[b, 0:8, :] = jnp.where(sublane == 0, stage[0, b:b + 1, :], pltpu.roll(proj[b, 64:72, :], 1, 0))
                proj[b, 72:80, :] = jnp.where(sublane == 7, stage[1, b:b + 1, :], pltpu.roll(proj[b, 8:16, :], 7, 0))
            staggered((tail_task(layer, lo, lo + TAIL // 64) for lo in range(0, blocks, TAIL // 64)), TAIL_WIDTH)

            @pl.when(layer < layers - 2)
            def _():
                send_halo(1 - slot)
            return carry

        def forecast(step, carry):
            def encode_task(dest, half):
                chunk = half * group + dest
                rows = pl.ds(pl.multiple_of(chunk * 256, 256), 256)
                feats = jnp.concatenate([xs[step, rows, :], xs[step + 1, rows, :]], axis=1)
                node = mlat[pl.ds(pl.multiple_of(chunk * 64, 64), 64), :]
                old = g2m[rows, :]
                pre = dot(feats, wg[step, 0:256, :]) + dot(fm[rows, :], wg[step, 256:384, :])
                yield
                y = dot(silu_of_half(pre), wembo[0])
                yield
                lat = norm(y).astype(BF16)
                glat[rows, :] = lat
                pre = dot(old, wei[0, 0:256, :]) + dot(lat, wei[0, 256:512, :])
                term = dot(node, wei[0, 512:768, :])
                yield
                pre = pre + jnp.concatenate([term] * 4, axis=0)
                y = dot(silu_of_half(pre), weo[0])
                yield
                edge = residual(old, norm(y)).astype(F32)
                return node, (edge[0:64] + edge[64:128] + edge[128:192] + edge[192:256]).astype(BF16)

            def encode_group(pairs):
                results = []

                def run(dest, half):
                    results.append((yield from encode_task(dest, half)))

                active = [run(dest, half) for dest, half in pairs]
                while active:
                    active = [task for task in active if next(task, "done") != "done"]
                    yield
                node = jnp.concatenate([r[0] for r in results], axis=0)
                esum = jnp.concatenate([r[1] for r in results], axis=0)
                pre = dot(node, wni[0, 0:256, :]) + dot(esum, wni[0, 256:512, :])
                yield
                y = dot(silu_of_half(pre), wno[0])
                yield
                new = residual(node, norm(y))
                for q, (dest, half) in enumerate(pairs):
                    hsend[half, dest] = new[q * 64:q * 64 + 64]

            def encode(it, carry):
                dests = [lax.rem(me + PER * it + 1 + q, group) for q in range(PER)]
                pairs = [(dest, half) for dest in dests for half in range(2)]
                staggered((encode_group(pairs[lo:lo + 4]) for lo in range(0, 2 * PER, 4)), 4)
                for q in range(PER - 1):
                    for half in range(2):
                        en_copy(PER * it + 1 + q, half).start()

                @pl.when(it < group // PER - 1)
                def _():
                    for half in range(2):
                        en_copy(PER * it + PER, half).start()
                return carry

            lax.fori_loop(0, group // PER, encode, 0)

            @pl.when(step == 0)
            def _():
                for half in range(2):
                    for hop in range(1, group):
                        ef_arrival(lax.rem(me + hop, group), half).wait_recv()
                    ef_keep(half).wait()

                def embed_edges(k, carry):
                    def edge_embed_task(sub):
                        def put(y):
                            ebase[k, sub * 64:sub * 64 + 256, :] = y.astype(BF16)
                        return plain_task(lambda: efl[sub:sub + 4].reshape(256, 128), put, wemb[3 + k], wembo[4])

                    together(edge_embed_task(sub) for sub in range(0, blocks, 4))
                    return carry

                lax.fori_loop(0, 6, embed_edges, 0)
                for hop in range(1, group):
                    for half in range(2):
                        ef_copy(hop, half).wait_send()

            elat[...] = ebase[...]
            for hop in range(1, group):
                for half in range(2):
                    en_arrival(lax.rem(me + hop, group), half).wait_recv()
            for hop in range(1, group):
                for half in range(2):
                    en_copy(hop, half).wait_send()
            hcur[...] = hin[...]
            for half in range(2):
                hcur[block_of(me, 1 + half)] = hsend[half, me]
            send_halo(1)
            put_projections(0, blocks, *project(1, 0, blocks))
            lax.fori_loop(1, layers - 1, mesh_layer, 0)
            for hop in range(1, group):
                for half in range(2):
                    de_copy(hop, half).start()
            for half in range(2):
                hd[half, me] = hcur[block_of(me, 1 + half)]

            def self_task(rows):
                old = glat[rows, :]

                def put(y):
                    gcur[rows, :] = residual(old, y)
                return plain_task(lambda: old, put, wsh[0], wgs[1])

            def self_update(it, carry):
                together(self_task(pl.ds(pl.multiple_of((it * 4 + sub) * 256, 256), 256)) for sub in range(4))
                return carry

            lax.fori_loop(0, 4, self_update, 0)

            def decode(it, carry):
                last = layers - 1
                for q in range(PER - 1):
                    for half in range(2):
                        de_arrival(lax.rem(me + PER * it + 1 + q, group), half).wait_recv()

                @pl.when(it < group // PER - 1)
                def _():
                    for half in range(2):
                        de_arrival(lax.rem(me + PER * it + PER, group), half).wait_recv()

                work = []
                for q in range(PER):
                    source = lax.rem(me + PER * it + 1 + q, group)
                    for half in range(2):
                        rows = pl.ds(pl.multiple_of((half * group + source) * 256, 256), 256)
                        work.append((rows, hd[half, source], m2g[rows, :], gcur[rows, :], xst[step, :, rows]))
                def decode_task(rows, node, old, grid, state):
                    pre = dot(old, wei[last, 0:256, :]) + dot(grid, wei[last, 512:768, :])
                    term = dot(node, wei[last, 256:512, :])
                    yield
                    pre = pre + jnp.concatenate([term] * 4, axis=0)
                    y = dot(silu_of_half(pre), weo[last])
                    yield
                    edge = residual(old, norm(y))
                    pre = dot(grid, wni[last, 0:256, :]) + dot(edge, wni[last, 256:512, :])
                    yield
                    y = dot(silu_of_half(pre), wno[last])
                    yield
                    out = residual(grid, norm(y))
                    pre = dot(out, wsh[1])
                    yield
                    hidden = dot(perms[1], silu_of_half(pre))
                    yield
                    p = dot_t(wof[...], hidden.astype(BF16))
                    yield
                    new = state + stats[:, 3:4] * p + stats[:, 2:3]
                    scaled = dot_t(perms[0], ((new - mean) / std).astype(BF16))
                    yield
                    xst[step + 1, :, rows] = new
                    xs[2, rows, 0:variables] = scaled.astype(BF16)

                staggered((decode_task(*args) for args in work), 2 * PER)
                return carry

            lax.fori_loop(0, group // PER, decode, 0)
            for hop in range(1, group):
                for half in range(2):
                    de_copy(hop, half).wait_send()

            @pl.when(step == 0)
            def _():
                pltpu.make_async_copy(xst.at[1], out0, osem.at[0]).start()
            return carry

        lax.fori_loop(0, 2, forecast, 0)
        final = pltpu.make_async_copy(xst.at[2], out1, osem.at[1])
        final.start()
        pltpu.make_async_copy(xst.at[1], out0, osem.at[0]).wait()
        final.wait()

    def local_run(x_prev, x_cur, forcing, grid_static, g2m_feat, m2g_feat, mesh_feat, mesh_edge_feat, norm_stats, w_grid_in, w_mesh_in, w_eemb_in, w_embed_out, w_edge_in, w_edge_out, w_node_in, w_node_out, w_grid_self, w_out_hidden, w_out_final):
        grid_dev, variables = x_prev.shape
        mesh_dev = mesh_feat.shape[0]
        latent = w_embed_out.shape[-1]
        blocks = 2 * group
        perms = jnp.asarray(row_permutation(), BF16)

        vmem = pl.BlockSpec(memory_space=pltpu.VMEM)
        anywhere = pl.BlockSpec(memory_space=pl.ANY)
        state = jax.ShapeDtypeStruct((variables, grid_dev), F32)
        dma = pltpu.SemaphoreType.DMA
        first, second = pl.pallas_call(
            kernel,
            out_shape=(state, state),
            in_specs=[anywhere, anywhere] + [vmem] * 12 + [anywhere] * 4 + [vmem] * 3,
            out_specs=(anywhere, anywhere),
            scratch_shapes=[
                pltpu.VMEM(w_edge_in.shape, BF16), pltpu.VMEM(w_edge_out.shape, BF16),
                pltpu.VMEM(w_node_in.shape, BF16), pltpu.VMEM(w_node_out.shape, BF16),
                pltpu.VMEM((3, variables, grid_dev), F32), pltpu.VMEM((3, grid_dev, 128), BF16), pltpu.VMEM((grid_dev, 128), BF16),
                pltpu.VMEM((grid_dev, latent), BF16), pltpu.VMEM((grid_dev, latent), BF16), pltpu.VMEM((grid_dev, latent), BF16),
                pltpu.VMEM((grid_dev, latent), BF16),
                pltpu.VMEM((mesh_dev, latent), BF16), pltpu.VMEM((blocks, 64, 128), BF16),
                pltpu.VMEM((6, mesh_dev, latent), BF16), pltpu.VMEM((6, mesh_dev, latent), BF16),
                pltpu.VMEM((2, group, 64, latent), BF16), pltpu.VMEM((blocks, 64, latent), BF16),
                pltpu.VMEM((blocks, 64, latent), BF16), pltpu.VMEM((2, group, 64, latent), BF16),
                pltpu.VMEM((blocks, 80, latent), F32), pltpu.VMEM((mesh_dev, latent), F32),
                pltpu.VMEM((2, 2, blocks, latent), BF16), pltpu.VMEM((2, 2, blocks, latent), BF16), pltpu.VMEM((2, blocks, latent), F32), pltpu.VMEM((2, latent, latent), BF16),
                pltpu.VMEM((2, 384, latent), BF16), pltpu.VMEM((9, 128, latent), BF16), pltpu.VMEM((2, 384, latent), F32),
                pltpu.VMEM((9, 128, latent), F32), pltpu.VMEM((-(-w_grid_in.shape[0] // 8) * 8, latent), F32),
                pltpu.VMEM((64, grid_dev), F32), pltpu.VMEM((8, mesh_dev), F32), pltpu.VMEM((48, mesh_dev), F32),
                pltpu.VMEM((8, grid_dev // 2), F32), pltpu.VMEM((8, mesh_dev // 2), F32), pltpu.VMEM((8, grid_dev // 2), F32),
                pltpu.VMEM((8, mesh_dev // 2), F32), pltpu.VMEM((2, group, 64, 128), BF16),
                dma((4,)), dma((2,)), dma((2,)), dma((2,)), dma((2,)), dma((group, 2)), dma((group, 2)), dma((group, 2)), dma((group, 2)),
                dma((group, 2)), dma((group, 2)), dma((2, 2)), dma((2, 2)),
            ],
            compiler_params=pltpu.CompilerParams(collective_id=0, has_side_effects=True, flags=FLAGS, vmem_limit_bytes=67043328),
        )(x_prev.T, x_cur.T, forcing.transpose(2, 1, 0), grid_static.T, g2m_feat.T, m2g_feat.T, mesh_feat.T, mesh_edge_feat.transpose(1, 2, 0),
          norm_stats.T, perms, w_grid_in, w_mesh_in, w_eemb_in, w_embed_out, w_edge_in, w_edge_out, w_node_in, w_node_out, w_grid_self,
          w_out_hidden, w_out_final.T)
        return first.T, second.T

    row_spec = P(("dp", "gp"))
    edge_spec = P(("dp", "gp"), None, None)
    whole = P()
    in_specs = (row_spec, row_spec, edge_spec, row_spec, row_spec, row_spec, row_spec, edge_spec, whole) + (whole,) * 11
    return jax.shard_map(local_run, mesh=mesh, in_specs=in_specs, out_specs=(row_spec, row_spec), check_vma=False)
```
